32 devices in a mesh: gx: 8 (over y, x, core), gy: 4 (over z).
Axes of the slice: x: 2, y: 2, z: 4, core: 2. Of those that a mesh axis runs over, the one named last changes fastest.
Arguments:
- right_side: float32 [32, 256, 256], P('gx', 'gy'), may hold values from -40 to 40
- kappa_sq: float32 [32, 256, 256], P('gx', 'gy'), may hold values from 0.5 to 4
Outputs:
- solution_field: float32 [32, 256, 256], P('gx', 'gy')
- residual: float32 [32, 256, 256], P('gx', 'gy')
- residual_rms: float32 [3], replicated
The draws below stay inside these ranges and needn't reach their ends.
All inputs are finite; a program needn't handle non-finite values.
Results may differ from the reference program's by a relative error of at most 0.00016.
Values sent between devices are 32-bit elements; how exact they have to be, the bound alone decides.
A program may use at most 64 MiB of HBM per device.

```python
import math
import jax
import jax.numpy as jnp

CZ = 256
ITERS = 3
NX = 32
NY = 256


def draw_right_side(key, part):
    first = jax.random.fold_in(key, 11)
    noise = jax.random.normal(first, (NX, NY, CZ), jnp.float32)
    place = jnp.arange(NX, dtype=jnp.float32) / NX
    rising = 1.0 + 2.0 * place
    values = noise * rising[:, None, None]
    return jnp.clip(values, -40.0, 40.0).astype(jnp.float32)


def level_of(key, shape, shards, least, largest):
    loudness = 1.0
    for axis_at, parts in shards:
        heights = jax.random.uniform(jax.random.fold_in(jax.random.fold_in(key, 6), axis_at), (parts,), jnp.float32, least / len(shards), largest / len(shards))
        loudness = loudness * jnp.repeat(jnp.exp(heights), shape[axis_at] // parts).reshape((-1,) + (1,) * (len(shape) - 1 - axis_at))
    return loudness


def setup_inputs(seed: int = 0) -> dict:
    key_of = jax.random.split(jax.random.key(seed), 3)
    return {
        "right_side": draw_right_side(jax.random.fold_in(key_of[2], 71), 0),
        "kappa_sq": jnp.clip(jnp.exp(math.log(4.0) - 2.0794415 * jax.random.uniform(key_of[1], (NX, NY, CZ), jnp.float32) ** level_of(key_of[1], (NX, NY, CZ), ((0, 8), (1, 4)), -0.2, 0.2)), 0.5, 4.0),
    }


def kpass(field, kappa_sq):
    beside = jnp.roll(field, 1, 0) + jnp.roll(field, -1, 0)
    beside = beside + jnp.roll(field, 1, 1) + jnp.roll(field, -1, 1)
    beside = beside + jnp.roll(field, 1, 2) + jnp.roll(field, -1, 2)
    return (6.0 + kappa_sq) * field - beside

def operate(field, kappa_sq):
    return kpass(kpass(field, kappa_sq), kappa_sq)

def reference(right_side, kappa_sq):
    shifted = 6.0 + kappa_sq
    precond = 1.0 / (shifted * shifted + 6.0)
    cells = right_side.shape[0] * right_side.shape[1] * right_side.shape[2]
    solution_field = jnp.zeros_like(right_side)
    residual = right_side
    u_vec = precond * residual
    w_vec = operate(u_vec, kappa_sq)
    p_vec = jnp.zeros_like(right_side)
    s_vec = jnp.zeros_like(right_side)
    q_vec = jnp.zeros_like(right_side)
    z_vec = jnp.zeros_like(right_side)
    norms = []
    gamma_old = jnp.float32(1.0)
    alpha_old = jnp.float32(1.0)
    for step in range(ITERS):
        gamma = jnp.sum(residual * u_vec)
        delta = jnp.sum(w_vec * u_vec)
        norm_sq = jnp.sum(residual * residual)
        norms.append(jnp.sqrt(norm_sq / cells))
        m_vec = precond * w_vec
        n_vec = operate(m_vec, kappa_sq)
        if step == 0:
            beta = jnp.float32(0.0)
            alpha = gamma / delta
        else:
            beta = gamma / gamma_old
            alpha = gamma / (delta - beta * gamma / alpha_old)
        z_vec = n_vec + beta * z_vec
        q_vec = m_vec + beta * q_vec
        s_vec = w_vec + beta * s_vec
        p_vec = u_vec + beta * p_vec
        solution_field = solution_field + alpha * p_vec
        residual = residual - alpha * s_vec
        u_vec = u_vec - alpha * q_vec
        w_vec = w_vec - alpha * z_vec
        gamma_old = gamma
        alpha_old = alpha
    return (solution_field, residual, jnp.stack(norms).astype(jnp.float32))
```

```python
import functools
import jax
import jax.numpy as jnp
from jax import lax
from jax.experimental import pallas as pl
from jax.experimental.pallas import tpu as pltpu
from jax.sharding import PartitionSpec as P

ITERS = 3
MESH = pl.DeviceIdType.MESH


def shifted(c):
    return [None] + c[:-1]


def plus(a, b, scale):
    out = []
    for one, two in zip(a, b):
        two = None if two is None else two * scale
        out.append(one if two is None else two if one is None else one + two)
    return out


def form(c, entry):
    total = None
    for i, one in enumerate(c):
        for j, two in enumerate(c):
            if one is not None and two is not None and i < ITERS and j < ITERS:
                term = one * two * entry(i, j)
                total = term if total is None else total + term
    return total


def coefficients(mu, dots, cells):
    one = jnp.ones_like(mu[0])
    res = [one] + [None] * ITERS
    step = [None] * (ITERS + 1)
    sol = [None] * (ITERS + 1)
    norms = []
    for i in range(ITERS):
        gamma = form(res, lambda a, b: mu[a + b])
        delta = form(res, lambda a, b: mu[a + b + 1])
        norms.append(jnp.sqrt(form(res, lambda a, b: dots[min(a, b), max(a, b)]) / cells))
        if i == 0:
            alpha = gamma / delta
            step = list(res)
        else:
            beta = gamma / gamma_old
            alpha = gamma / (delta - beta * gamma / alpha_old)
            step = plus(res, step, beta)
        sol = plus(sol, step, alpha)
        res = plus(res, shifted(step), -alpha)
        gamma_old, alpha_old = gamma, alpha
    return sol, res, norms


FACES = ("y0", "t0", "d", "y1", "t1", "w1", "t2")
SLOT = {name: i for i, name in enumerate(FACES)}
OUTER, INNER_ROW, INNER_LAYER, PARTIAL = 1, 2, 3, 4


def kernel(
    nx, ny, cells, rhs_hbm, kappa_hbm, *refs,
):
    (
    v_ref, y_ref, coef_ref, t_ref, f_ref, w_ref, d_ref, m_ref, pre_ref, face_ref, edge_out, edge_in,
    corner_out, corner_in, slots, load_sem, face_send, face_recv, edge_send, edge_recv,
    corner_send, corner_recv, sum_send, sum_recv,
    ) = refs
    layers, rows, cols = rhs_hbm.shape
    assert layers >= 3 and rows >= 3
    ix, iy = lax.axis_index("gx"), lax.axis_index("gy")
    count = nx * ny
    me = ix * ny + iy
    ends, seconds = (0, layers - 1), (1, layers - 2)
    order = [0, layers - 1] + list(range(1, layers - 1))
    inside = list(range(1, layers - 1))
    loads = {}
    for l in order:
        loads[l] = (
            pltpu.make_async_copy(kappa_hbm.at[l], d_ref.at[l], load_sem.at[0, l]),
            pltpu.make_async_copy(rhs_hbm.at[l], v_ref.at[0, l], load_sem.at[1, l]),
        )
        for copy in loads[l]:
            copy.start()

    barrier = pltpu.get_barrier_semaphore()
    x_of = (lax.rem(ix + nx - 1, nx), lax.rem(ix + 1, nx))
    y_of = (lax.rem(iy + ny - 1, ny), lax.rem(iy + 1, ny))

    near = ny // 2 <= 2

    def greet(x, y):
        pl.semaphore_signal(barrier, inc=1, device_id=(x, y), device_id_type=MESH)

    def greet_any(k, carry):
        other = lax.rem(me + k, count)
        greet(other // ny, lax.rem(other, ny))
        return carry

    def greet_x(k, carry):
        greet(lax.rem(ix + k, nx), iy)
        return carry

    def greet_y(k, carry):
        greet(ix, lax.rem(iy + k, ny))
        return carry

    if near:
        for x in x_of:
            for y in y_of:
                greet(x, y)
        lax.fori_loop(1, ny, greet_y, 0)
        lax.fori_loop(1, nx, greet_x, 0)
        greetings = nx - 1 + ny - 1 + 4
    else:
        lax.fori_loop(1, count, greet_any, 0)
        greetings = count - 1

    row = lax.broadcasted_iota(jnp.int32, (rows, cols), 0)
    first, last = row == 0, row == rows - 1

    def across(x):
        return pltpu.roll(x, 1, 1) + pltpu.roll(x, cols - 1, 1)

    def lateral(x):
        up = jnp.where(first, 0.0, pltpu.roll(x, 1, 0))
        down = jnp.where(last, 0.0, pltpu.roll(x, rows - 1, 0))
        return across(x) + (up + down)

    def local_k(get, l):
        x = get(l)
        out = d_ref[l] * x - lateral(x)
        if l > 0:
            out = out - get(l - 1)
        if l < layers - 1:
            out = out - get(l + 1)
        return out

    def tile_sum(x):
        return jnp.sum(x, axis=(0, 1), keepdims=True)

    def dot(a, b):
        return tile_sum(sum(a(l) * b(l) for l in range(layers)))

    at = [pl.ds((0, rows - 1)[side], 1) for side in range(2)]
    at_second = [pl.ds((1, rows - 2)[side], 1) for side in range(2)]
    sends = []

    def remote(src, dst, send, recv, device):
        copy = pltpu.make_async_remote_copy(
            src_ref=src, dst_ref=dst, send_sem=send, recv_sem=recv,
            device_id=device, device_id_type=MESH,
        )
        sends.append(copy)
        return copy

    def edges(name, src):
        n = SLOT[name]
        out = []
        for side in range(2):
            for l in range(layers):
                edge_out[n, side, l] = src[l, at[side], :]
        for side in range(2):
            copy = remote(
                edge_out.at[n, side], edge_in.at[n, 1 - side],
                edge_send.at[n, side], edge_recv.at[n, 1 - side], (ix, y_of[side]),
            )
            copy.start()
            out.append(copy)
        return out

    def faces(name, src):
        n = SLOT[name]
        out = []
        for k in range(2):
            copy = remote(
                src.at[ends[k]], face_ref.at[n, 1 - k],
                face_send.at[n, k], face_recv.at[n, 1 - k], (x_of[k], iy),
            )
            copy.start()
            out.append(copy)
        return out

    def corners(n, start, size):
        out = []
        for k in range(2):
            for side in range(2):
                q, there = 2 * k + side, 2 * (1 - k) + 1 - side
                copy = remote(
                    corner_out.at[q, pl.ds(start, size)], corner_in.at[there, pl.ds(start, size)],
                    corner_send.at[n, q], corner_recv.at[n, there], (x_of[k], y_of[side]),
                )
                copy.start()
                out.append(copy)
        return out

    def arrive(copies):
        for copy in copies:
            copy.wait_recv()

    def edge(name, side, l):
        return edge_in[SLOT[name], side, l]

    def face(name, k):
        return face_ref[SLOT[name], k]

    def corner(k, side, part):
        return corner_in[2 * k + side, part]

    mu, dots = ([], {})

    def full_t(j):
        for l in range(layers):
            t = t_ref[j, l]
            for k in range(2):
                if l == ends[k]:
                    t = t - face(f"y{j}", k)
            f_ref[l] = t
            for side in range(2):
                f_ref[l, at[side], :] = f_ref[l, at[side], :] - edge(f"y{j}", side, l)
        mu.append(dot(lambda l: f_ref[l], lambda l: f_ref[l]))

    def next_v(j):
        for l in order:
            v = local_k(lambda n: f_ref[n], l)
            if l in ends:
                v = v + y_ref[j, l]
            v_ref[j + 1, l] = v
            for side in range(2):
                v_ref[j + 1, l, at[side], :] = v_ref[j + 1, l, at[side], :] + y_ref[j, l, at[side], :]

    def next_rows(j, part):
        for l in order:
            for side in range(2):
                line = v_ref[j + 1, l, at[side], :] - edge(f"t{j}", side, l)
                for k in range(2):
                    if l == ends[k]:
                        line = line + 2.0 * corner(k, side, part)
                v_ref[j + 1, l, at[side], :] = line

    for l in order:
        for copy in loads[l]:
            copy.wait()
        d = 6.0 + d_ref[l]
        d_ref[l] = d
        m_ref[l] = 1.0 / (d * d + 6.0)
        y_ref[0, l] = m_ref[l] * v_ref[0, l]
    pl.semaphore_wait(barrier, greetings)
    y_edges = edges("y0", y_ref.at[0])
    for k in range(2):
        for side in range(2):
            corner_out[2 * k + side, 0] = y_ref[0, ends[k], at[side], :]
    y_corners = corners(0, 0, 1)
    y_faces = faces("y0", y_ref.at[0])
    for l in order:
        t_ref[0, l] = local_k(lambda n: y_ref[0, n], l)
    t_edges = edges("t0", t_ref.at[0])
    t_faces = faces("t0", t_ref.at[0])
    d_edges = edges("d", d_ref)
    d_faces = faces("d", d_ref)
    mu.append(dot(lambda l: v_ref[0, l], lambda l: y_ref[0, l]))
    dots[0, 0] = dot(lambda l: v_ref[0, l], lambda l: v_ref[0, l])
    arrive(y_edges + y_faces)
    full_t(0)
    next_v(0)
    arrive(t_edges + y_corners)
    next_rows(0, 0)
    for l in inside:
        y_ref[1, l] = m_ref[l] * v_ref[1, l]
    arrive(t_faces)
    for k in range(2):
        v = v_ref[1, ends[k]] - face("t0", k)
        v_ref[1, ends[k]] = v
        y_ref[1, ends[k]] = m_ref[ends[k]] * v
    y_edges = edges("y1", y_ref.at[1])
    for k in range(2):
        for side in range(2):
            q = 2 * k + side
            corner_out[q, OUTER] = y_ref[1, ends[k], at[side], :]
            corner_out[q, INNER_ROW] = y_ref[1, ends[k], at_second[side], :]
            corner_out[q, INNER_LAYER] = y_ref[1, seconds[k], at[side], :]
    y_corners = corners(1, OUTER, 3)
    y_faces = faces("y1", y_ref.at[1])
    for l in order:
        t_ref[1, l] = local_k(lambda n: y_ref[1, n], l)
    t_edges = edges("t1", t_ref.at[1])
    for k in range(2):
        for side in range(2):
            corner_out[2 * k + side, PARTIAL] = t_ref[1, ends[k], at[side], :]
    t_corners = corners(2, PARTIAL, 1)
    t_faces = faces("t1", t_ref.at[1])
    for l in order:
        w_ref[l] = local_k(lambda n: t_ref[1, n], l)
    w_edges = edges("w1", w_ref)
    w_faces = faces("w1", w_ref)
    mu.append(dot(lambda l: v_ref[1, l], lambda l: y_ref[1, l]))
    for i in range(2):
        dots[i, 1] = dot(lambda l: v_ref[i, l], lambda l: v_ref[1, l])
    arrive(y_edges + y_faces)
    full_t(1)
    next_v(1)
    arrive(t_edges + y_corners + t_corners + d_edges)
    next_rows(1, OUTER)
    for l in inside:
        y_ref[2, l] = m_ref[l] * v_ref[2, l]
    past = {
        (k, side): corner(k, side, PARTIAL) - (edge("y1", side, ends[k]) + face_ref[SLOT["y1"], k, at[side], :])
        for k in range(2)
        for side in range(2)
    }
    edge_part = {}
    for side in range(2):
        lines = []
        for l in range(layers):
            line = y_ref[1, l, at[side], :]
            for k in range(2):
                if l == ends[k]:
                    line = line + corner(k, side, OUTER)
            lines.append(line)
        for l in range(layers):
            beside = across(lines[l])
            if l > 0:
                beside = beside + lines[l - 1]
            if l < layers - 1:
                beside = beside + lines[l + 1]
            part = beside - edge("d", side, l) * lines[l] - f_ref[l, at[side], :]
            for k in range(2):
                if l == ends[k]:
                    part = part + (corner(k, side, INNER_ROW) - past[k, side])
            edge_part[side, l] = part
    arrive(d_faces)
    for k in range(2):
        pre_ref[k] = y_ref[1, ends[k]]
        for side in range(2):
            pre_ref[k, at[side], :] = pre_ref[k, at[side], :] + corner(k, side, OUTER)
        a = pre_ref[k]
        pre_ref[k] = lateral(a) - face("d", k) * a - f_ref[ends[k]]
        for side in range(2):
            pre_ref[k, at[side], :] = pre_ref[k, at[side], :] + (corner(k, side, INNER_LAYER) - past[k, side])
    arrive(t_faces)
    for k in range(2):
        v = v_ref[2, ends[k]] - face("t1", k)
        v_ref[2, ends[k]] = v
        y_ref[2, ends[k]] = m_ref[ends[k]] * v
    for l in order:
        t_ref[2, l] = local_k(lambda n: y_ref[2, n], l)
    mu.append(dot(lambda l: v_ref[2, l], lambda l: y_ref[2, l]))
    for i in range(3):
        dots[i, 2] = dot(lambda l: v_ref[i, l], lambda l: v_ref[2, l])
    arrive(w_edges)
    for side in range(2):
        for l in range(layers):
            d = edge("d", side, l)
            y = (edge("w1", side, l) + edge_part[side, l]) / (d * d + 6.0)
            t_ref[2, l, at[side], :] = t_ref[2, l, at[side], :] - y
    arrive(w_faces)
    for k in range(2):
        d = face("d", k)
        y = (face("w1", k) + pre_ref[k]) / (d * d + 6.0)
        t_ref[2, ends[k]] = t_ref[2, ends[k]] - y
    mu.append(dot(lambda l: t_ref[2, l], lambda l: t_ref[2, l]))
    start_sums(mu, dots, slots, sum_send, sum_recv, me, nx, ny)
    t_edges = edges("t2", t_ref.at[2])
    t_faces = faces("t2", t_ref.at[2])
    for l in order:
        v_ref[3, l] = local_k(lambda n: t_ref[2, n], l)
    arrive(t_edges)
    for l in range(layers):
        for side in range(2):
            v_ref[3, l, at[side], :] = v_ref[3, l, at[side], :] - edge("t2", side, l)
    arrive(t_faces)
    for k in range(2):
        v_ref[3, ends[k]] = v_ref[3, ends[k]] - face("t2", k)

    for copy in sends:
        copy.wait_send()
    all_slots = slots.at[pl.ds(0, count - 1)]
    pltpu.make_async_copy(all_slots, all_slots, sum_send).wait()
    pltpu.make_async_copy(all_slots, all_slots, sum_recv).wait()
    total = jnp.sum(slots[...], axis=0)
    names = [("mu", i) for i in range(2 * ITERS)] + sorted(dots)
    got = {
        name: jnp.broadcast_to(total[:, k : k + 1], total.shape) for k, name in enumerate(names)
    }
    mu = [got["mu", i] for i in range(2 * ITERS)]
    sol, res, norms = coefficients(mu, got, float(cells))
    for k, value in enumerate(norms + sol[:ITERS] + res[1:]):
        coef_ref[k] = value[0, 0]


def start_sums(mu, dots, slots, sum_send, sum_recv, me, nx, ny):
    lane = lax.broadcasted_iota(jnp.int32, (1, slots.shape[-1]), 1)
    line = jnp.zeros(lane.shape, jnp.float32)
    for k, value in enumerate(mu + [dots[name] for name in sorted(dots)]):
        line = jnp.where(lane == k, value, line)
    slots[me] = line

    def send(x, y):
        pltpu.make_async_remote_copy(
            src_ref=slots.at[me],
            dst_ref=slots.at[me],
            send_sem=sum_send,
            recv_sem=sum_recv,
            device_id=(x, y),
            device_id_type=MESH,
        ).start()

    ix, iy = lax.axis_index("gx"), lax.axis_index("gy")
    y_at = [lax.rem(iy + k, ny) for k in range(ny)]

    def send_line(k, carry):
        x = ix + k
        x = jnp.where(x >= nx, x - nx, x)
        for y in y_at[1:] + y_at[:1]:
            send(x, y)
        return carry

    lax.fori_loop(1, nx, send_line, 0)
    for y in y_at[1:]:
        send(ix, y)


def finish(coef, v_ref, y_ref, sol_ref, res_ref, norms_ref):
    for i in range(ITERS):
        norms_ref[i] = coef[i]
    for l in range(v_ref.shape[1]):
        sol = coef[ITERS] * y_ref[0, l]
        res = v_ref[0, l]
        for i in range(1, ITERS):
            sol = sol + coef[ITERS + i] * y_ref[i, l]
        for i in range(1, ITERS + 1):
            res = res + coef[2 * ITERS + i - 1] * v_ref[i, l]
        sol_ref[l] = sol
        res_ref[l] = res


def body(right_side, kappa_sq):
    nx, ny = lax.axis_size("gx"), lax.axis_size("gy")
    shape = right_side.shape
    layers, rows, cols = shape
    cells = nx * layers * ny * rows * cols
    f32 = jnp.float32
    dma = pltpu.SemaphoreType.DMA
    whole = pl.BlockSpec(memory_space=pltpu.VMEM)
    smem = pl.BlockSpec(memory_space=pltpu.SMEM)
    out = pl.pallas_call(
        functools.partial(kernel, nx, ny, cells),
        out_shape=(
            pltpu.VMEM((ITERS + 1,) + shape, f32),
            pltpu.VMEM((ITERS,) + shape, f32),
            pltpu.SMEM((3 * ITERS,), f32),
        ),
        in_specs=[pl.BlockSpec(memory_space=pl.ANY)] * 2,
        out_specs=(whole, whole, smem),
        scratch_shapes=[
            pltpu.VMEM((ITERS,) + shape, f32),
            pltpu.VMEM(shape, f32),
            pltpu.VMEM(shape, f32),
            pltpu.VMEM(shape, f32),
            pltpu.VMEM(shape, f32),
            pltpu.VMEM((2, rows, cols), f32),
            pltpu.VMEM((len(FACES), 2, rows, cols), f32),
            pltpu.VMEM((len(FACES), 2, layers, 1, cols), f32),
            pltpu.VMEM((len(FACES), 2, layers, 1, cols), f32),
            pltpu.VMEM((4, 5, 1, cols), f32),
            pltpu.VMEM((4, 5, 1, cols), f32),
            pltpu.VMEM((nx * ny, 1, 128), f32),
            dma((2, layers)),
            dma((len(FACES), 2)),
            dma((len(FACES), 2)),
            dma((len(FACES), 2)),
            dma((len(FACES), 2)),
            dma((3, 4)),
            dma((3, 4)),
            dma(()),
            dma(()),
        ],
        compiler_params=pltpu.CompilerParams(collective_id=0, has_side_effects=True),
    )(right_side, kappa_sq)
    return pl.pallas_call(
        finish,
        out_shape=(
            jax.ShapeDtypeStruct(shape, f32),
            jax.ShapeDtypeStruct(shape, f32),
            jax.ShapeDtypeStruct((ITERS,), f32),
        ),
        in_specs=[smem, whole, whole],
        out_specs=(whole, whole, smem),
    )(out[2], *(pltpu.with_memory_space_constraint(x, pltpu.VMEM) for x in out[:2]))


def solution(mesh):
    return jax.shard_map(
        body,
        mesh=mesh,
        in_specs=(P("gx", "gy", None), P("gx", "gy", None)),
        out_specs=(P("gx", "gy", None), P("gx", "gy", None), P()),
        check_vma=False,
    )
```

```python
import functools
import jax
import jax.numpy as jnp
from jax import lax
from jax.experimental import pallas as pl
from jax.experimental.pallas import tpu as pltpu
from jax.sharding import PartitionSpec as P

ITERS = 3
MESH = pl.DeviceIdType.MESH


def shifted(c):
    return [None] + c[:-1]


def plus(a, b, scale):
    out = []
    for one, two in zip(a, b):
        two = None if two is None else two * scale
        out.append(one if two is None else two if one is None else one + two)
    return out


def form(c, entry):
    total = None
    for i, one in enumerate(c):
        for j, two in enumerate(c):
            if one is not None and two is not None and i < ITERS and j < ITERS:
                term = one * two * entry(i, j)
                total = term if total is None else total + term
    return total


def coefficients(mu, dots, cells):
    one = jnp.ones_like(mu[0])
    res = [one] + [None] * ITERS
    step = [None] * (ITERS + 1)
    sol = [None] * (ITERS + 1)
    norms = []
    for i in range(ITERS):
        gamma = form(res, lambda a, b: mu[a + b])
        delta = form(res, lambda a, b: mu[a + b + 1])
        norms.append(jnp.sqrt(form(res, lambda a, b: dots[min(a, b), max(a, b)]) / cells))
        if i == 0:
            alpha = gamma / delta
            step = list(res)
        else:
            beta = gamma / gamma_old
            alpha = gamma / (delta - beta * gamma / alpha_old)
            step = plus(res, step, beta)
        sol = plus(sol, step, alpha)
        res = plus(res, shifted(step), -alpha)
        gamma_old, alpha_old = gamma, alpha
    return sol, res, norms


FACES = ("y0", "t0", "d", "y1", "t1", "w1", "t2")
SLOT = {name: i for i, name in enumerate(FACES)}
TILE = 8
OUTER, INNER_ROW, INNER_LAYER, PARTIAL, LAST = 1, 2, 3, 4, 5


def kernel(
    nx, ny, cells, rhs_hbm, kappa_hbm, *refs,
):
    (
    v_ref, y_ref, coef_ref, t_ref, f_ref, w_ref, d_ref, m_ref, pre_ref, near_m, face_ref, edge_out, edge_in,
    corner_out, corner_in, slots, load_sem, face_send, face_recv, edge_send, edge_recv,
    corner_send, corner_recv, sum_send, sum_recv,
    ) = refs
    layers, rows, cols = rhs_hbm.shape
    assert layers >= 3 and rows % TILE == 0 and rows >= 6 * TILE
    cut_w = rows // (4 * TILE) * TILE
    cut_t, cut_y, cut = cut_w + TILE, cut_w + 2 * TILE, cut_w + 3 * TILE
    ix, iy = lax.axis_index("gx"), lax.axis_index("gy")
    count = nx * ny
    me = ix * ny + iy
    ends, seconds = (0, layers - 1), (1, layers - 2)
    order = [0, layers - 1] + list(range(1, layers - 1))
    inside = list(range(1, layers - 1))
    loads = {}
    for l in order:
        loads[l] = (
            pltpu.make_async_copy(kappa_hbm.at[l], d_ref.at[l], load_sem.at[0, l]),
            pltpu.make_async_copy(rhs_hbm.at[l], v_ref.at[0, l], load_sem.at[1, l]),
        )
        for copy in loads[l]:
            copy.start()

    barrier = pltpu.get_barrier_semaphore()
    x_of = (lax.rem(ix + nx - 1, nx), lax.rem(ix + 1, nx))
    y_of = (lax.rem(iy + ny - 1, ny), lax.rem(iy + 1, ny))

    near = ny // 2 <= 2

    def greet(x, y):
        pl.semaphore_signal(barrier, inc=1, device_id=(x, y), device_id_type=MESH)

    def greet_any(k, carry):
        other = lax.rem(me + k, count)
        greet(other // ny, lax.rem(other, ny))
        return carry

    def greet_x(k, carry):
        greet(lax.rem(ix + k, nx), iy)
        return carry

    def greet_y(k, carry):
        greet(ix, lax.rem(iy + k, ny))
        return carry

    if near:
        for x in x_of:
            for y in y_of:
                greet(x, y)
        lax.fori_loop(1, ny, greet_y, 0)
        lax.fori_loop(1, nx, greet_x, 0)
        greetings = nx - 1 + ny - 1 + 4
    else:
        lax.fori_loop(1, count, greet_any, 0)
        greetings = count - 1

    row = lax.broadcasted_iota(jnp.int32, (rows, cols), 0)
    first, last = row == 0, row == rows - 1

    def across(x):
        return pltpu.roll(x, 1, 1) + pltpu.roll(x, cols - 1, 1)

    def lateral(x):
        up = jnp.where(first, 0.0, pltpu.roll(x, 1, 0))
        down = jnp.where(last, 0.0, pltpu.roll(x, rows - 1, 0))
        return across(x) + (up + down)

    def local_k(ref, l, lo=0, hi=rows):
        a, b = max(lo - TILE, 0), min(hi + TILE, rows)
        x = ref[l, a:b]
        up, down = pltpu.roll(x, 1, 0), pltpu.roll(x, b - a - 1, 0)
        if a == 0:
            up = jnp.where(row[: b - a] == 0, 0.0, up)
        if b == rows:
            down = jnp.where(row[: b - a] == b - a - 1, 0.0, down)
        mid = slice(lo - a, hi - a)
        x = x[mid]
        out = d_ref[l, lo:hi] * x - (across(x) + (up[mid] + down[mid]))
        if l > 0:
            out = out - ref[l - 1, lo:hi]
        if l < layers - 1:
            out = out - ref[l + 1, lo:hi]
        return out

    def tile_sum(x):
        return jnp.sum(x, axis=(0, 1), keepdims=True)

    def dot(a, b):
        return tile_sum(sum(a(l) * b(l) for l in range(layers)))

    at = [pl.ds((0, rows - 1)[side], 1) for side in range(2)]
    at_second = [pl.ds((1, rows - 2)[side], 1) for side in range(2)]
    sends = []

    def remote(src, dst, send, recv, device):
        copy = pltpu.make_async_remote_copy(
            src_ref=src, dst_ref=dst, send_sem=send, recv_sem=recv,
            device_id=device, device_id_type=MESH,
        )
        sends.append(copy)
        return copy

    def edges(name, src, side):
        n = SLOT[name]
        for l in range(layers):
            edge_out[n, side, l] = src[l, at[side], :]
        copy = remote(
            edge_out.at[n, side], edge_in.at[n, 1 - side],
            edge_send.at[n, side], edge_recv.at[n, 1 - side], (ix, y_of[side]),
        )
        copy.start()
        return [copy]

    def faces(name, src, part, lo, hi):
        n = SLOT[name]
        out = []
        for k in range(2):
            copy = remote(
                src.at[ends[k], pl.ds(lo, hi - lo)], face_ref.at[n, 1 - k, pl.ds(lo, hi - lo)],
                face_send.at[n, part, k], face_recv.at[n, part, 1 - k], (x_of[k], iy),
            )
            copy.start()
            out.append(copy)
        return out

    def corners(n, side, start, size):
        out = []
        for k in range(2):
            q, there = 2 * k + side, 2 * (1 - k) + 1 - side
            copy = remote(
                corner_out.at[q, pl.ds(start, size)], corner_in.at[there, pl.ds(start, size)],
                corner_send.at[n, q], corner_recv.at[n, there], (x_of[k], y_of[side]),
            )
            copy.start()
            out.append(copy)
        return out

    def arrive(copies):
        for copy in copies:
            copy.wait_recv()

    def edge(name, side, l):
        return edge_in[SLOT[name], side, l]

    def face(name, k):
        return face_ref[SLOT[name], k]

    def corner(k, side, part):
        return corner_in[2 * k + side, part]

    mu, dots = ([], {})

    def full_t(j, lo, hi):
        for l in range(layers):
            t = t_ref[j, l, lo:hi]
            for k in range(2):
                if l == ends[k]:
                    t = t - face_ref[SLOT[f"y{j}"], k, lo:hi]
            f_ref[l, lo:hi] = t
            for side in range(2):
                if (0, rows)[side] in (lo, hi):
                    f_ref[l, at[side], :] = f_ref[l, at[side], :] - edge(f"y{j}", side, l)

    def next_v(j, lo, hi):
        for l in order:
            v = local_k(f_ref, l, lo, hi)
            if l in ends:
                v = v + y_ref[j, l, lo:hi]
            v_ref[j + 1, l, lo:hi] = v
            for side in range(2):
                if (0, rows)[side] in (lo, hi):
                    line = y_ref[j, l, at[side], :]
                    v_ref[j + 1, l, at[side], :] = v_ref[j + 1, l, at[side], :] + line

    def next_rows(j, part, sides):
        for l in order:
            for side in sides:
                line = v_ref[j + 1, l, at[side], :] - edge(f"t{j}", side, l)
                for k in range(2):
                    if l == ends[k]:
                        line = line + 2.0 * corner(k, side, part)
                v_ref[j + 1, l, at[side], :] = line

    def next_y(j, which, lo, hi):
        for l in which:
            y_ref[j, l, lo:hi] = m_ref[l, lo:hi] * v_ref[j, l, lo:hi]

    def next_ends(j, lo, hi):
        for k in range(2):
            l = ends[k]
            v = v_ref[j + 1, l, lo:hi] - face_ref[SLOT[f"t{j}"], k, lo:hi]
            v_ref[j + 1, l, lo:hi] = v
            y_ref[j + 1, l, lo:hi] = m_ref[l, lo:hi] * v

    for l in order:
        for copy in loads[l]:
            copy.wait()
        d = 6.0 + d_ref[l]
        d_ref[l] = d
        m_ref[l] = 1.0 / (d * d + 6.0)
        y_ref[0, l] = m_ref[l] * v_ref[0, l]
    pl.semaphore_wait(barrier, greetings)
    y, t = y_ref.at[0], t_ref.at[0]
    got = {}
    for side in range(2):
        got["ye", 1 - side] = edges("y0", y, side)
        for k in range(2):
            corner_out[2 * k + side, 0] = y[ends[k], at[side], :]
        got["yc", 1 - side] = corners(0, side, 0, 1)
    got["y", 0] = faces("y0", y, 0, 0, cut)
    for l in order:
        t[l] = local_k(y, l)
    got["t", 0] = faces("t0", t, 0, 0, cut)
    for side in range(2):
        got["te", 1 - side] = edges("t0", t, side)
    got["y", 1] = faces("y0", y, 1, cut, rows)
    got["t", 1] = faces("t0", t, 1, cut, rows)
    mu.append(dot(lambda l: v_ref[0, l], lambda l: y_ref[0, l]))
    dots[0, 0] = dot(lambda l: v_ref[0, l], lambda l: v_ref[0, l])
    y, t = y_ref.at[1], t_ref.at[1]
    y_edges, y_corners, y_faces = [], [], []
    t_edges, t_corners, t_faces = [], [], []
    w_edges, w_faces = [], []
    spans = [
        [(0, cut), (0, cut_y), (0, cut_t), (0, cut_w)],
        [(cut, rows), (cut_y, rows), (cut_t, rows), (cut_w, rows)],
    ]
    for part in range(2):
        side, (span, span_y, span_t, span_w) = part, spans[part]
        arrive(got["ye", side])
        if part == 0:
            d_edges = edges("d", d_ref, 0) + edges("d", d_ref, 1)
            d_faces = faces("d", d_ref, 0, 0, rows)
        arrive(got["y", part])
        full_t(0, *span)
        next_v(0, *span_y)
        arrive(got["te", side] + got["yc", side])
        next_rows(0, 0, (side,))
        next_y(1, inside, *span_y)
        arrive(got["t", part])
        next_ends(0, *span_y)
        y_faces += faces("y1", y, part, *span_y)
        y_edges += edges("y1", y, side)
        for k in range(2):
            q = 2 * k + side
            corner_out[q, OUTER] = y[ends[k], at[side], :]
            corner_out[q, INNER_ROW] = y[ends[k], at_second[side], :]
            corner_out[q, INNER_LAYER] = y[seconds[k], at[side], :]
        y_corners += corners(1, side, OUTER, 3)
        lo, hi = span_t
        for l in order:
            t[l, lo:hi] = local_k(y, l, lo, hi)
        t_faces += faces("t1", t, part, lo, hi)
        t_edges += edges("t1", t, side)
        for k in range(2):
            corner_out[2 * k + side, PARTIAL] = t[ends[k], at[side], :]
        t_corners += corners(2, side, PARTIAL, 1)
        lo, hi = span_w
        for l in order:
            w_ref[l, lo:hi] = local_k(t, l, lo, hi)
        w_faces += faces("w1", w_ref, part, lo, hi)
        w_edges += edges("w1", w_ref, side)
    mu.append(dot(lambda l: f_ref[l], lambda l: f_ref[l]))
    mu.append(dot(lambda l: v_ref[1, l], lambda l: y_ref[1, l]))
    for i in range(2):
        dots[i, 1] = dot(lambda l: v_ref[i, l], lambda l: v_ref[1, l])
    arrive(y_edges + y_faces)
    full_t(1, 0, rows)
    next_v(1, 0, rows)
    mu.append(dot(lambda l: f_ref[l], lambda l: f_ref[l]))
    arrive(t_edges + y_corners + t_corners + d_edges)
    next_rows(1, OUTER, range(2))
    next_y(2, inside, 0, rows)
    past = {
        (k, side): corner(k, side, PARTIAL) - (edge("y1", side, ends[k]) + face_ref[SLOT["y1"], k, at[side], :])
        for k in range(2)
        for side in range(2)
    }
    edge_part = {}
    for side in range(2):
        lines = []
        for l in range(layers):
            line = y_ref[1, l, at[side], :]
            for k in range(2):
                if l == ends[k]:
                    line = line + corner(k, side, OUTER)
            lines.append(line)
        for l in range(layers):
            beside = across(lines[l])
            if l > 0:
                beside = beside + lines[l - 1]
            if l < layers - 1:
                beside = beside + lines[l + 1]
            part = beside - edge("d", side, l) * lines[l] - f_ref[l, at[side], :]
            for k in range(2):
                if l == ends[k]:
                    part = part + (corner(k, side, INNER_ROW) - past[k, side])
            edge_part[side, l] = part
    arrive(d_faces)
    for k in range(2):
        pre_ref[k] = y_ref[1, ends[k]]
        for side in range(2):
            pre_ref[k, at[side], :] = pre_ref[k, at[side], :] + corner(k, side, OUTER)
        a = pre_ref[k]
        d = face("d", k)
        near_m[k] = 1.0 / (d * d + 6.0)
        pre_ref[k] = lateral(a) - d * a - f_ref[ends[k]]
        for side in range(2):
            pre_ref[k, at[side], :] = pre_ref[k, at[side], :] + (corner(k, side, INNER_LAYER) - past[k, side])
    arrive(t_faces)
    next_ends(1, 0, rows)
    y, t = y_ref.at[2], t_ref.at[2]
    y_corners, t_edges = [], []
    for side in range(2):
        for k in range(2):
            corner_out[2 * k + side, LAST] = y[ends[k], at[side], :]
        y_corners += corners(3, side, LAST, 1)
    for l in order:
        t[l] = local_k(y, l)
        f_ref[l] = t[l]
    for side in range(2):
        t_edges += edges("t2", t, side)
    t_faces = faces("t2", t, 0, 0, rows)
    mu.append(dot(lambda l: v_ref[2, l], lambda l: y_ref[2, l]))
    for i in range(3):
        dots[i, 2] = dot(lambda l: v_ref[i, l], lambda l: v_ref[2, l])
    arrive(w_edges)
    for side in range(2):
        for l in range(layers):
            d = edge("d", side, l)
            y = (edge("w1", side, l) + edge_part[side, l]) / (d * d + 6.0)
            f_ref[l, at[side], :] = f_ref[l, at[side], :] - y
    part = sum(f_ref[l] * f_ref[l] for l in inside)
    line = sums_line(mu, dots, slots.shape[-1])
    arrive(w_faces)
    for k in range(2):
        t = f_ref[ends[k]] - near_m[k] * (face("w1", k) + pre_ref[k])
        f_ref[ends[k]] = t
        part = part + t * t
    mu.append(tile_sum(part))
    lane = lax.broadcasted_iota(jnp.int32, line.shape, 1)
    slots[me] = jnp.where(lane == place(("mu", 2 * ITERS - 1)), mu[-1], line)
    start_sums(slots, sum_send, sum_recv, me, nx, ny)
    next_v(2, 0, rows)
    arrive(t_edges + y_corners)
    next_rows(2, LAST, range(2))
    arrive(t_faces)
    for k in range(2):
        v_ref[3, ends[k]] = v_ref[3, ends[k]] - face("t2", k)

    for copy in sends:
        copy.wait_send()
    all_slots = slots.at[pl.ds(0, count - 1)]
    pltpu.make_async_copy(all_slots, all_slots, sum_send).wait()
    pltpu.make_async_copy(all_slots, all_slots, sum_recv).wait()
    total = jnp.sum(slots[...], axis=0)

    def whole(name):
        n = place(name)
        return jnp.broadcast_to(total[:, n : n + 1], total.shape)

    mu = [whole(("mu", i)) for i in range(2 * ITERS)]
    got = {name: whole(name) for name in dots}
    sol, res, norms = coefficients(mu, got, float(cells))
    for k, value in enumerate(norms + sol[:ITERS] + res[1:]):
        coef_ref[k] = value[0, 0]


def place(name):
    names = [("mu", i) for i in range(2 * ITERS)]
    names += [(i, j) for j in range(ITERS) for i in range(j + 1)]
    return names.index(name)


def sums_line(mu, dots, size):
    lane = lax.broadcasted_iota(jnp.int32, (1, size), 1)
    line = jnp.zeros(lane.shape, jnp.float32)
    named = [(("mu", i), value) for i, value in enumerate(mu)] + list(dots.items())
    for name, value in named:
        line = jnp.where(lane == place(name), value, line)
    return line


def start_sums(slots, sum_send, sum_recv, me, nx, ny):
    def send(x, y):
        pltpu.make_async_remote_copy(
            src_ref=slots.at[me],
            dst_ref=slots.at[me],
            send_sem=sum_send,
            recv_sem=sum_recv,
            device_id=(x, y),
            device_id_type=MESH,
        ).start()

    ix, iy = lax.axis_index("gx"), lax.axis_index("gy")
    y_at = [lax.rem(iy + k, ny) for k in range(ny)]

    def send_line(k, carry):
        x = ix + k
        x = jnp.where(x >= nx, x - nx, x)
        for y in y_at[1:] + y_at[:1]:
            send(x, y)
        return carry

    lax.fori_loop(1, nx, send_line, 0)
    for y in y_at[1:]:
        send(ix, y)


def finish(coef, v_ref, y_ref, sol_ref, res_ref, norms_ref):
    for i in range(ITERS):
        norms_ref[i] = coef[i]
    for l in range(v_ref.shape[1]):
        sol = coef[ITERS] * y_ref[0, l]
        res = v_ref[0, l]
        for i in range(1, ITERS):
            sol = sol + coef[ITERS + i] * y_ref[i, l]
        for i in range(1, ITERS + 1):
            res = res + coef[2 * ITERS + i - 1] * v_ref[i, l]
        sol_ref[l] = sol
        res_ref[l] = res


def body(right_side, kappa_sq):
    nx, ny = lax.axis_size("gx"), lax.axis_size("gy")
    shape = right_side.shape
    layers, rows, cols = shape
    cells = nx * layers * ny * rows * cols
    f32 = jnp.float32
    dma = pltpu.SemaphoreType.DMA
    whole = pl.BlockSpec(memory_space=pltpu.VMEM)
    smem = pl.BlockSpec(memory_space=pltpu.SMEM)
    out = pl.pallas_call(
        functools.partial(kernel, nx, ny, cells),
        out_shape=(
            pltpu.VMEM((ITERS + 1,) + shape, f32),
            pltpu.VMEM((ITERS,) + shape, f32),
            pltpu.SMEM((3 * ITERS,), f32),
        ),
        in_specs=[pl.BlockSpec(memory_space=pl.ANY)] * 2,
        out_specs=(whole, whole, smem),
        scratch_shapes=[
            pltpu.VMEM((ITERS,) + shape, f32),
            pltpu.VMEM(shape, f32),
            pltpu.VMEM(shape, f32),
            pltpu.VMEM(shape, f32),
            pltpu.VMEM(shape, f32),
            pltpu.VMEM((2, rows, cols), f32),
            pltpu.VMEM((2, rows, cols), f32),
            pltpu.VMEM((len(FACES), 2, rows, cols), f32),
            pltpu.VMEM((len(FACES), 2, layers, 1, cols), f32),
            pltpu.VMEM((len(FACES), 2, layers, 1, cols), f32),
            pltpu.VMEM((4, 6, 1, cols), f32),
            pltpu.VMEM((4, 6, 1, cols), f32),
            pltpu.VMEM((nx * ny, 1, 128), f32),
            dma((2, layers)),
            dma((len(FACES), 2, 2)),
            dma((len(FACES), 2, 2)),
            dma((len(FACES), 2)),
            dma((len(FACES), 2)),
            dma((4, 4)),
            dma((4, 4)),
            dma(()),
            dma(()),
        ],
        compiler_params=pltpu.CompilerParams(collective_id=0, has_side_effects=True),
    )(right_side, kappa_sq)
    return pl.pallas_call(
        finish,
        out_shape=(
            jax.ShapeDtypeStruct(shape, f32),
            jax.ShapeDtypeStruct(shape, f32),
            jax.ShapeDtypeStruct((ITERS,), f32),
        ),
        in_specs=[smem, whole, whole],
        out_specs=(whole, whole, smem),
    )(out[2], *(pltpu.with_memory_space_constraint(x, pltpu.VMEM) for x in out[:2]))


def solution(mesh):
    return jax.shard_map(
        body,
        mesh=mesh,
        in_specs=(P("gx", "gy", None), P("gx", "gy", None)),
        out_specs=(P("gx", "gy", None), P("gx", "gy", None), P()),
        check_vma=False,
    )
```

```python
import functools
import jax
import jax.numpy as jnp
from jax import lax
from jax.experimental import pallas as pl
from jax.experimental.pallas import tpu as pltpu
from jax.sharding import PartitionSpec as P

ITERS = 3
MESH = pl.DeviceIdType.MESH


def shifted(c):
    return [None] + c[:-1]


def plus(a, b, scale):
    out = []
    for one, two in zip(a, b):
        two = None if two is None else two * scale
        out.append(one if two is None else two if one is None else one + two)
    return out


def form(c, entry):
    total = None
    for i, one in enumerate(c):
        for j, two in enumerate(c):
            if one is not None and two is not None and i < ITERS and j < ITERS:
                term = one * two * entry(i, j)
                total = term if total is None else total + term
    return total


def coefficients(mu, dots, cells):
    one = jnp.ones_like(mu[0])
    res = [one] + [None] * ITERS
    step = [None] * (ITERS + 1)
    sol = [None] * (ITERS + 1)
    norms = []
    for i in range(ITERS):
        gamma = form(res, lambda a, b: mu[a + b])
        delta = form(res, lambda a, b: mu[a + b + 1])
        norms.append(jnp.sqrt(form(res, lambda a, b: dots[min(a, b), max(a, b)]) / cells))
        if i == 0:
            alpha = gamma / delta
            step = list(res)
        else:
            beta = gamma / gamma_old
            alpha = gamma / (delta - beta * gamma / alpha_old)
            step = plus(res, step, beta)
        sol = plus(sol, step, alpha)
        res = plus(res, shifted(step), -alpha)
        gamma_old, alpha_old = gamma, alpha
    return sol, res, norms


FACES = ("y0", "t0", "d", "y1", "t1", "w1", "t2")
SLOT = {name: i for i, name in enumerate(FACES)}
SAME = {"t2": "y0"}
SPLIT = ("y0", "t0")
ARRIVALS = tuple((name, part) for name in SPLIT for part in range(2)) + tuple(
    (name, 0) for name in ("d", "y1", "t1", "w1")
)
TILE = 8
OUTER, INNER_ROW, INNER_LAYER, PARTIAL, LAST = 1, 2, 3, 4, 5


def kernel(
    nx, ny, cells, rhs_hbm, kappa_hbm, *refs,
):
    (
    v_ref, y_ref, coef_ref, t_ref, f_ref, w_ref, d_ref, m_ref, pre_ref, near_m, face_ref, edge_out, edge_in,
    corner_out, corner_in, slots, load_sem, face_send, face_recv, edge_send, edge_recv,
    corner_send, corner_recv, sum_send, sum_recv,
    ) = refs
    layers, rows, cols = rhs_hbm.shape
    assert layers >= 3 and rows % TILE == 0 and rows >= 6 * TILE
    cut_w = rows // (4 * TILE) * TILE
    cut_t, cut_y, cut = cut_w + TILE, cut_w + 2 * TILE, cut_w + 3 * TILE
    ix, iy = lax.axis_index("gx"), lax.axis_index("gy")
    count = nx * ny
    me = ix * ny + iy
    ends, seconds = (0, layers - 1), (1, layers - 2)
    order = [0, layers - 1] + list(range(1, layers - 1))
    inside = list(range(1, layers - 1))
    load_k = pltpu.make_async_copy(kappa_hbm, d_ref, load_sem.at[0])
    load_r = pltpu.make_async_copy(rhs_hbm, v_ref.at[0], load_sem.at[1])
    load_k.start()
    load_r.start()

    barrier = pltpu.get_barrier_semaphore()
    x_of = (lax.rem(ix + nx - 1, nx), lax.rem(ix + 1, nx))
    y_of = (lax.rem(iy + ny - 1, ny), lax.rem(iy + 1, ny))

    near = ny // 2 <= 2

    def greet(x, y):
        pl.semaphore_signal(barrier, inc=1, device_id=(x, y), device_id_type=MESH)

    def greet_any(k, carry):
        other = lax.rem(me + k, count)
        greet(other // ny, lax.rem(other, ny))
        return carry

    def greet_x(k, carry):
        greet(lax.rem(ix + k, nx), iy)
        return carry

    def greet_y(k, carry):
        greet(ix, lax.rem(iy + k, ny))
        return carry

    if near:
        for x in x_of:
            for y in y_of:
                greet(x, y)
        lax.fori_loop(1, ny, greet_y, 0)
        lax.fori_loop(1, nx, greet_x, 0)
        greetings = nx - 1 + ny - 1 + 4
    else:
        lax.fori_loop(1, count, greet_any, 0)
        greetings = count - 1

    row = lax.broadcasted_iota(jnp.int32, (rows, cols), 0)
    first, last = row == 0, row == rows - 1

    def across(x):
        return pltpu.roll(x, 1, 1) + pltpu.roll(x, cols - 1, 1)

    def lateral(x):
        up = jnp.where(first, 0.0, pltpu.roll(x, 1, 0))
        down = jnp.where(last, 0.0, pltpu.roll(x, rows - 1, 0))
        return across(x) + (up + down)

    def local_k(ref, l, lo=0, hi=rows):
        a, b = max(lo - TILE, 0), min(hi + TILE, rows)
        x = ref[l, a:b]
        up, down = pltpu.roll(x, 1, 0), pltpu.roll(x, b - a - 1, 0)
        if a == 0:
            up = jnp.where(row[: b - a] == 0, 0.0, up)
        if b == rows:
            down = jnp.where(row[: b - a] == b - a - 1, 0.0, down)
        mid = slice(lo - a, hi - a)
        x = x[mid]
        out = d_ref[l, lo:hi] * x - (across(x) + (up[mid] + down[mid]))
        if l > 0:
            out = out - ref[l - 1, lo:hi]
        if l < layers - 1:
            out = out - ref[l + 1, lo:hi]
        return out

    def tile_sum(x):
        return jnp.sum(x, axis=(0, 1), keepdims=True)

    def dot(a, b):
        return tile_sum(sum(a(l) * b(l) for l in range(layers)))

    at = [pl.ds((0, rows - 1)[side], 1) for side in range(2)]
    at_second = [pl.ds((1, rows - 2)[side], 1) for side in range(2)]
    def remote(src, dst, send, recv, device):
        pltpu.make_async_remote_copy(
            src_ref=src, dst_ref=dst, send_sem=send, recv_sem=recv,
            device_id=device, device_id_type=MESH,
        ).start()

    def wait(ref, sem):
        pltpu.make_async_copy(ref, ref, sem).wait()

    def edge_sem(name, side):
        return edge_recv.at[ARRIVALS.index((name, side if name in SPLIT else 0))]

    def edges(name, src, side):
        n = SLOT[name]
        for l in range(layers):
            edge_out[n, side, l] = src[l, at[side], :]
        sem = edge_sem(SAME.get(name, name), 1 - side)
        remote(edge_out.at[n, side], edge_in.at[n, 1 - side], edge_send, sem, (ix, y_of[side]))

    def wait_edges(name, side=None):
        if side is None:
            wait(edge_in.at[SLOT[name]], edge_sem(name, 0))
        else:
            wait(edge_in.at[SLOT[name], side], edge_sem(SAME.get(name, name), side))

    def face_sem(name, part):
        return face_recv.at[ARRIVALS.index((name, part if name in SPLIT else 0))]

    def faces(name, src, part, lo, hi):
        n, span = SLOT[name], pl.ds(lo, hi - lo)
        sem = face_sem(SAME.get(name, name), part)
        for k in range(2):
            remote(
                src.at[ends[k], span], face_ref.at[n, 1 - k, span], face_send, sem, (x_of[k], iy)
            )

    def wait_faces(name, part=0, lo=0, hi=rows):
        sem = face_sem(SAME.get(name, name), part)
        wait(face_ref.at[SLOT[name], :, pl.ds(lo, hi - lo)], sem)

    def corners(side, start, size, again=True):
        sem = corner_recv.at[1 - side if again else 2]
        for k in range(2):
            span = pl.ds(start, size)
            remote(
                corner_out.at[side, k, span], corner_in.at[1 - side, 1 - k, span],
                corner_send, sem, (x_of[k], y_of[side]),
            )

    def edge(name, side, l):
        return edge_in[SLOT[name], side, l]

    def face(name, k):
        return face_ref[SLOT[name], k]

    def corner(k, side, part):
        return corner_in[side, k, part]

    mu, dots = ([], {})

    def full_t(j, lo, hi):
        for l in range(layers):
            t = t_ref[j, l, lo:hi]
            for k in range(2):
                if l == ends[k]:
                    t = t - face_ref[SLOT[f"y{j}"], k, lo:hi]
            f_ref[l, lo:hi] = t
            for side in range(2):
                if (0, rows)[side] in (lo, hi):
                    f_ref[l, at[side], :] = f_ref[l, at[side], :] - edge(f"y{j}", side, l)

    def next_v(j, lo, hi):
        for l in order:
            v = local_k(f_ref, l, lo, hi)
            if l in ends:
                v = v + y_ref[j, l, lo:hi]
            v_ref[j + 1, l, lo:hi] = v
            for side in range(2):
                if (0, rows)[side] in (lo, hi):
                    line = y_ref[j, l, at[side], :]
                    v_ref[j + 1, l, at[side], :] = v_ref[j + 1, l, at[side], :] + line

    def next_rows(j, part, sides):
        for l in order:
            for side in sides:
                line = v_ref[j + 1, l, at[side], :] - edge(f"t{j}", side, l)
                for k in range(2):
                    if l == ends[k]:
                        line = line + 2.0 * corner(k, side, part)
                v_ref[j + 1, l, at[side], :] = line

    def next_y(j, which, lo, hi):
        for l in which:
            y_ref[j, l, lo:hi] = m_ref[l, lo:hi] * v_ref[j, l, lo:hi]

    def next_ends(j, lo, hi):
        for k in range(2):
            l = ends[k]
            v = v_ref[j + 1, l, lo:hi] - face_ref[SLOT[f"t{j}"], k, lo:hi]
            v_ref[j + 1, l, lo:hi] = v
            y_ref[j + 1, l, lo:hi] = m_ref[l, lo:hi] * v

    load_k.wait()
    for l in order:
        d = 6.0 + d_ref[l]
        d_ref[l] = d
        m_ref[l] = 1.0 / (d * d + 6.0)
    load_r.wait()
    for l in order:
        y_ref[0, l] = m_ref[l] * v_ref[0, l]
    pl.semaphore_wait(barrier, greetings)
    y, t = y_ref.at[0], t_ref.at[0]
    for side in range(2):
        edges("y0", y, side)
        for k in range(2):
            corner_out[side, k, 0] = y[ends[k], at[side], :]
        corners(side, 0, 1)
    faces("y0", y, 0, 0, cut)
    for l in order:
        t[l] = local_k(y, l)
    faces("t0", t, 0, 0, cut)
    for side in range(2):
        edges("t0", t, side)
    faces("y0", y, 1, cut, rows)
    faces("t0", t, 1, cut, rows)
    mu.append(dot(lambda l: v_ref[0, l], lambda l: y_ref[0, l]))
    dots[0, 0] = dot(lambda l: v_ref[0, l], lambda l: v_ref[0, l])
    y, t = y_ref.at[1], t_ref.at[1]
    spans = [
        [(0, cut), (0, cut_y), (0, cut_t), (0, cut_w)],
        [(cut, rows), (cut_y, rows), (cut_t, rows), (cut_w, rows)],
    ]
    for part in range(2):
        side, (span, span_y, span_t, span_w) = part, spans[part]
        wait_edges("y0", side)
        if part == 0:
            edges("d", d_ref, 0)
            edges("d", d_ref, 1)
            faces("d", d_ref, 0, 0, rows)
        wait_faces("y0", part, *span)
        full_t(0, *span)
        next_v(0, *span_y)
        wait_edges("t0", side)
        wait(corner_in.at[side, :, 0], corner_recv.at[side])
        next_rows(0, 0, (side,))
        next_y(1, inside, *span_y)
        wait_faces("t0", part, *span)
        next_ends(0, *span_y)
        faces("y1", y, part, *span_y)
        edges("y1", y, side)
        for k in range(2):
            corner_out[side, k, OUTER] = y[ends[k], at[side], :]
            corner_out[side, k, INNER_ROW] = y[ends[k], at_second[side], :]
            corner_out[side, k, INNER_LAYER] = y[seconds[k], at[side], :]
        corners(side, OUTER, 3, False)
        lo, hi = span_t
        for l in order:
            t[l, lo:hi] = local_k(y, l, lo, hi)
        faces("t1", t, part, lo, hi)
        edges("t1", t, side)
        for k in range(2):
            corner_out[side, k, PARTIAL] = t[ends[k], at[side], :]
        corners(side, PARTIAL, 1, False)
        lo, hi = span_w
        for l in order:
            w_ref[l, lo:hi] = local_k(t, l, lo, hi)
        faces("w1", w_ref, part, lo, hi)
        edges("w1", w_ref, side)
    mu.append(dot(lambda l: f_ref[l], lambda l: f_ref[l]))
    mu.append(dot(lambda l: v_ref[1, l], lambda l: y_ref[1, l]))
    for i in range(2):
        dots[i, 1] = dot(lambda l: v_ref[i, l], lambda l: v_ref[1, l])
    wait_edges("y1")
    wait_faces("y1")
    full_t(1, 0, rows)
    next_v(1, 0, rows)
    mu.append(dot(lambda l: f_ref[l], lambda l: f_ref[l]))
    wait_edges("t1")
    wait_edges("d")
    wait(corner_in.at[:, :, pl.ds(OUTER, 4)], corner_recv.at[2])
    next_rows(1, OUTER, range(2))
    next_y(2, inside, 0, rows)
    past = {
        (k, side): corner(k, side, PARTIAL) - (edge("y1", side, ends[k]) + face_ref[SLOT["y1"], k, at[side], :])
        for k in range(2)
        for side in range(2)
    }
    edge_part = {}
    for side in range(2):
        lines = []
        for l in range(layers):
            line = y_ref[1, l, at[side], :]
            for k in range(2):
                if l == ends[k]:
                    line = line + corner(k, side, OUTER)
            lines.append(line)
        for l in range(layers):
            beside = across(lines[l])
            if l > 0:
                beside = beside + lines[l - 1]
            if l < layers - 1:
                beside = beside + lines[l + 1]
            part = beside - edge("d", side, l) * lines[l] - f_ref[l, at[side], :]
            for k in range(2):
                if l == ends[k]:
                    part = part + (corner(k, side, INNER_ROW) - past[k, side])
            edge_part[side, l] = part
    wait_faces("d")
    for k in range(2):
        pre_ref[k] = y_ref[1, ends[k]]
        for side in range(2):
            pre_ref[k, at[side], :] = pre_ref[k, at[side], :] + corner(k, side, OUTER)
        a = pre_ref[k]
        d = face("d", k)
        near_m[k] = 1.0 / (d * d + 6.0)
        pre_ref[k] = lateral(a) - d * a - f_ref[ends[k]]
        for side in range(2):
            pre_ref[k, at[side], :] = pre_ref[k, at[side], :] + (corner(k, side, INNER_LAYER) - past[k, side])
    wait_faces("t1")
    next_ends(1, 0, rows)
    y, t = y_ref.at[2], t_ref.at[2]
    for side in range(2):
        for k in range(2):
            corner_out[side, k, LAST] = y[ends[k], at[side], :]
        corners(side, LAST, 1)
    for l in order:
        t[l] = local_k(y, l)
        f_ref[l] = t[l]
    for side in range(2):
        edges("t2", t, side)
    faces("t2", t, 0, 0, rows)
    mu.append(dot(lambda l: v_ref[2, l], lambda l: y_ref[2, l]))
    for i in range(3):
        dots[i, 2] = dot(lambda l: v_ref[i, l], lambda l: v_ref[2, l])
    wait_edges("w1")
    for side in range(2):
        for l in range(layers):
            d = edge("d", side, l)
            y = (edge("w1", side, l) + edge_part[side, l]) / (d * d + 6.0)
            f_ref[l, at[side], :] = f_ref[l, at[side], :] - y
    part = sum(f_ref[l] * f_ref[l] for l in inside)
    line = sums_line(mu, dots, slots.shape[-1])
    wait_faces("w1")
    for k in range(2):
        t = f_ref[ends[k]] - near_m[k] * (face("w1", k) + pre_ref[k])
        f_ref[ends[k]] = t
        part = part + t * t
    mu.append(tile_sum(part))
    lane = lax.broadcasted_iota(jnp.int32, line.shape, 1)
    slots[me] = jnp.where(lane == place(("mu", 2 * ITERS - 1)), mu[-1], line)
    start_sums(slots, sum_send, sum_recv, me, nx, ny)
    next_v(2, 0, rows)
    for side in range(2):
        wait_edges("t2", side)
        wait(corner_in.at[side, :, LAST], corner_recv.at[side])
    next_rows(2, LAST, range(2))
    wait_faces("t2")
    for k in range(2):
        v_ref[3, ends[k]] = v_ref[3, ends[k]] - face("t2", k)

    wait(face_ref, face_send)
    wait(edge_in, edge_send)
    wait(corner_in, corner_send)
    all_slots = slots.at[pl.ds(0, count - 1)]
    pltpu.make_async_copy(all_slots, all_slots, sum_send).wait()
    pltpu.make_async_copy(all_slots, all_slots, sum_recv).wait()
    total = jnp.sum(slots[...], axis=0)

    def whole(name):
        n = place(name)
        return jnp.broadcast_to(total[:, n : n + 1], total.shape)

    mu = [whole(("mu", i)) for i in range(2 * ITERS)]
    got = {name: whole(name) for name in dots}
    sol, res, norms = coefficients(mu, got, float(cells))
    for k, value in enumerate(norms + sol[:ITERS] + res[1:]):
        coef_ref[k] = value[0, 0]


def place(name):
    names = [("mu", i) for i in range(2 * ITERS)]
    names += [(i, j) for j in range(ITERS) for i in range(j + 1)]
    return names.index(name)


def sums_line(mu, dots, size):
    lane = lax.broadcasted_iota(jnp.int32, (1, size), 1)
    line = jnp.zeros(lane.shape, jnp.float32)
    named = [(("mu", i), value) for i, value in enumerate(mu)] + list(dots.items())
    for name, value in named:
        line = jnp.where(lane == place(name), value, line)
    return line


def start_sums(slots, sum_send, sum_recv, me, nx, ny):
    def send(x, y):
        pltpu.make_async_remote_copy(
            src_ref=slots.at[me],
            dst_ref=slots.at[me],
            send_sem=sum_send,
            recv_sem=sum_recv,
            device_id=(x, y),
            device_id_type=MESH,
        ).start()

    ix, iy = lax.axis_index("gx"), lax.axis_index("gy")
    y_at = [lax.rem(iy + k, ny) for k in range(ny)]

    def send_line(k, carry):
        x = ix + k
        x = jnp.where(x >= nx, x - nx, x)
        for y in y_at[1:] + y_at[:1]:
            send(x, y)
        return carry

    lax.fori_loop(1, nx, send_line, 0)
    for y in y_at[1:]:
        send(ix, y)


def finish(coef, v_ref, y_ref, sol_ref, res_ref, norms_ref):
    for i in range(ITERS):
        norms_ref[i] = coef[i]
    for l in range(v_ref.shape[1]):
        sol = coef[ITERS] * y_ref[0, l]
        res = v_ref[0, l]
        for i in range(1, ITERS):
            sol = sol + coef[ITERS + i] * y_ref[i, l]
        for i in range(1, ITERS + 1):
            res = res + coef[2 * ITERS + i - 1] * v_ref[i, l]
        sol_ref[l] = sol
        res_ref[l] = res


def body(right_side, kappa_sq):
    nx, ny = lax.axis_size("gx"), lax.axis_size("gy")
    shape = right_side.shape
    layers, rows, cols = shape
    cells = nx * layers * ny * rows * cols
    f32 = jnp.float32
    dma = pltpu.SemaphoreType.DMA
    whole = pl.BlockSpec(memory_space=pltpu.VMEM)
    smem = pl.BlockSpec(memory_space=pltpu.SMEM)
    out = pl.pallas_call(
        functools.partial(kernel, nx, ny, cells),
        out_shape=(
            pltpu.VMEM((ITERS + 1,) + shape, f32),
            pltpu.VMEM((ITERS,) + shape, f32),
            pltpu.SMEM((3 * ITERS,), f32),
        ),
        in_specs=[pl.BlockSpec(memory_space=pl.ANY)] * 2,
        out_specs=(whole, whole, smem),
        scratch_shapes=[
            pltpu.VMEM((ITERS,) + shape, f32),
            pltpu.VMEM(shape, f32),
            pltpu.VMEM(shape, f32),
            pltpu.VMEM(shape, f32),
            pltpu.VMEM(shape, f32),
            pltpu.VMEM((2, rows, cols), f32),
            pltpu.VMEM((2, rows, cols), f32),
            pltpu.VMEM((len(FACES), 2, rows, cols), f32),
            pltpu.VMEM((len(FACES), 2, layers, 1, cols), f32),
            pltpu.VMEM((len(FACES), 2, layers, 1, cols), f32),
            pltpu.VMEM((2, 2, 6, 1, cols), f32),
            pltpu.VMEM((2, 2, 6, 1, cols), f32),
            pltpu.VMEM((nx * ny, 1, 128), f32),
            dma((2,)),
            dma(()),
            dma((len(ARRIVALS),)),
            dma(()),
            dma((len(ARRIVALS),)),
            dma(()),
            dma((3,)),
            dma(()),
            dma(()),
        ],
        compiler_params=pltpu.CompilerParams(collective_id=0, has_side_effects=True),
    )(right_side, kappa_sq)
    return pl.pallas_call(
        finish,
        out_shape=(
            jax.ShapeDtypeStruct(shape, f32),
            jax.ShapeDtypeStruct(shape, f32),
            jax.ShapeDtypeStruct((ITERS,), f32),
        ),
        in_specs=[smem, whole, whole],
        out_specs=(whole, whole, smem),
    )(out[2], *(pltpu.with_memory_space_constraint(x, pltpu.VMEM) for x in out[:2]))


def solution(mesh):
    return jax.shard_map(
        body,
        mesh=mesh,
        in_specs=(P("gx", "gy", None), P("gx", "gy", None)),
        out_specs=(P("gx", "gy", None), P("gx", "gy", None), P()),
        check_vma=False,
    )
```

```python
import functools
import jax
import jax.numpy as jnp
from jax import lax
from jax.experimental import pallas as pl
from jax.experimental.pallas import tpu as pltpu
from jax.sharding import PartitionSpec as P

ITERS = 3
MESH = pl.DeviceIdType.MESH


def shifted(c):
    return [None] + c[:-1]


def plus(a, b, scale):
    out = []
    for one, two in zip(a, b):
        two = None if two is None else two * scale
        out.append(one if two is None else two if one is None else one + two)
    return out


def form(c, entry):
    total = None
    for i, one in enumerate(c):
        for j, two in enumerate(c):
            if one is not None and two is not None and i < ITERS and j < ITERS:
                term = one * two * entry(i, j)
                total = term if total is None else total + term
    return total


def coefficients(mu, dots, cells):
    one = jnp.ones_like(mu[0])
    res = [one] + [None] * ITERS
    step = [None] * (ITERS + 1)
    sol = [None] * (ITERS + 1)
    norms = []
    for i in range(ITERS):
        gamma = form(res, lambda a, b: mu[a + b])
        delta = form(res, lambda a, b: mu[a + b + 1])
        norms.append(jnp.sqrt(form(res, lambda a, b: dots[min(a, b), max(a, b)]) / cells))
        if i == 0:
            alpha = gamma / delta
            step = list(res)
        else:
            beta = gamma / gamma_old
            alpha = gamma / (delta - beta * gamma / alpha_old)
            step = plus(res, step, beta)
        sol = plus(sol, step, alpha)
        res = plus(res, shifted(step), -alpha)
        gamma_old, alpha_old = gamma, alpha
    return sol, res, norms


FACES = ("y0", "t0", "y1", "d", "t1", "w1", "t2")
SLOT = {name: i for i, name in enumerate(FACES)}
SAME = {"t2": "y0"}
SPLIT = ("y0", "t0")
ARRIVALS = tuple((name, part) for name in SPLIT for part in range(2)) + tuple(
    (name, 0) for name in ("y1", "t1", "w1", "d")
)
TILE = 8
OUTER, INNER_ROW, INNER_LAYER, PARTIAL, LAST = 1, 2, 3, 4, 5


def kernel(
    nx, ny, cells, rhs_hbm, kappa_hbm, *refs,
):
    (
    v_ref, y_ref, coef_ref, t_ref, f_ref, w_ref, d_ref, m_ref, pre_ref, near_m, face_ref, edge_out, edge_in,
    corner_out, corner_in, slots, load_sem, face_recv, edge_send, edge_recv,
    corner_recv, sum_send, sum_recv,
    ) = refs
    layers, rows, cols = rhs_hbm.shape
    assert layers >= 3 and rows % TILE == 0 and rows >= 6 * TILE
    cut_w = rows // (4 * TILE) * TILE
    cut_t, cut_y, cut = cut_w + TILE, cut_w + 2 * TILE, cut_w + 3 * TILE
    ix, iy = lax.axis_index("gx"), lax.axis_index("gy")
    count = nx * ny
    me = ix * ny + iy
    ends, seconds = (0, layers - 1), (1, layers - 2)
    order = [0, layers - 1] + list(range(1, layers - 1))
    inside = list(range(1, layers - 1))
    face_send, corner_send = load_sem.at[0], load_sem.at[1]
    load_k = pltpu.make_async_copy(kappa_hbm, d_ref, load_sem.at[0])
    load_r = pltpu.make_async_copy(rhs_hbm, v_ref.at[0], load_sem.at[1])
    load_k.start()
    load_r.start()

    barrier = pltpu.get_barrier_semaphore()
    x_of = (lax.rem(ix + nx - 1, nx), lax.rem(ix + 1, nx))
    y_of = (lax.rem(iy + ny - 1, ny), lax.rem(iy + 1, ny))

    near = ny // 2 <= 2

    def greet(x, y):
        pl.semaphore_signal(barrier, inc=1, device_id=(x, y), device_id_type=MESH)

    def greet_any(k, carry):
        other = lax.rem(me + k, count)
        greet(other // ny, lax.rem(other, ny))
        return carry

    def greet_x(k, carry):
        greet(lax.rem(ix + k, nx), iy)
        return carry

    def greet_y(k, carry):
        greet(ix, lax.rem(iy + k, ny))
        return carry

    if near:
        for x in x_of:
            greet(x, iy)
        for y in y_of:
            for x in x_of:
                greet(x, y)
        lax.fori_loop(1, ny, greet_y, 0)
        lax.fori_loop(2, nx - 1, greet_x, 0)
        greetings = nx - 1 + ny - 1 + 4
    else:
        lax.fori_loop(1, count, greet_any, 0)
        greetings = count - 1

    row = lax.broadcasted_iota(jnp.int32, (rows, cols), 0)
    first, last = row == 0, row == rows - 1

    def across(x):
        return pltpu.roll(x, 1, 1) + pltpu.roll(x, cols - 1, 1)

    def lateral(x):
        up = jnp.where(first, 0.0, pltpu.roll(x, 1, 0))
        down = jnp.where(last, 0.0, pltpu.roll(x, rows - 1, 0))
        return across(x) + (up + down)

    def local_k(ref, l, lo=0, hi=rows):
        a, b = max(lo - TILE, 0), min(hi + TILE, rows)
        x = ref[l, a:b]
        up, down = pltpu.roll(x, 1, 0), pltpu.roll(x, b - a - 1, 0)
        if a == 0:
            up = jnp.where(row[: b - a] == 0, 0.0, up)
        if b == rows:
            down = jnp.where(row[: b - a] == b - a - 1, 0.0, down)
        mid = slice(lo - a, hi - a)
        x = x[mid]
        out = d_ref[l, lo:hi] * x - (across(x) + (up[mid] + down[mid]))
        if l > 0:
            out = out - ref[l - 1, lo:hi]
        if l < layers - 1:
            out = out - ref[l + 1, lo:hi]
        return out

    def tile_sum(x):
        return jnp.sum(x, axis=(0, 1), keepdims=True)

    def dot(a, b):
        return tile_sum(sum(a(l) * b(l) for l in range(layers)))

    at = [pl.ds((0, rows - 1)[side], 1) for side in range(2)]
    at_second = [pl.ds((1, rows - 2)[side], 1) for side in range(2)]
    def remote(src, dst, send, recv, device):
        pltpu.make_async_remote_copy(
            src_ref=src, dst_ref=dst, send_sem=send, recv_sem=recv,
            device_id=device, device_id_type=MESH,
        ).start()

    def wait(ref, sem):
        pltpu.make_async_copy(ref, ref, sem).wait()

    def edge_sem(name, side):
        return edge_recv.at[ARRIVALS.index((name, side if name in SPLIT else 0))]

    def stage(name, src, side):
        for l in range(layers):
            edge_out[SLOT[name], side, l] = src[l, at[side], :]

    def edges(name, src, side):
        n = SLOT[name]
        if name != "y0":
            stage(name, src, side)
        sem = edge_sem("t1" if name == "d" else SAME.get(name, name), 1 - side)
        remote(edge_out.at[n, side], edge_in.at[n, 1 - side], edge_send, sem, (ix, y_of[side]))

    def wait_edges(name, side=None):
        if side is None:
            wait(edge_in.at[SLOT[name]], edge_sem(name, 0))
        else:
            wait(edge_in.at[SLOT[name], side], edge_sem(SAME.get(name, name), side))

    def face_sem(name, part):
        return face_recv.at[ARRIVALS.index((name, part if name in SPLIT else 0))]

    def faces(name, src, part, lo, hi):
        n, span = SLOT[name], pl.ds(lo, hi - lo)
        sem = face_sem(SAME.get(name, name), part)
        for k in range(2):
            remote(
                src.at[ends[k], span], face_ref.at[n, 1 - k, span], face_send, sem, (x_of[k], iy)
            )

    def wait_faces(name, part=0, lo=0, hi=rows):
        sem = face_sem(SAME.get(name, name), part)
        wait(face_ref.at[SLOT[name], :, pl.ds(lo, hi - lo)], sem)

    def corners(side, start, size, again=True):
        sem = corner_recv.at[1 - side if again else 2]
        for k in range(2):
            span = pl.ds(start, size)
            remote(
                corner_out.at[side, k, span], corner_in.at[1 - side, 1 - k, span],
                corner_send, sem, (x_of[k], y_of[side]),
            )

    def edge(name, side, l):
        return edge_in[SLOT[name], side, l]

    def face(name, k):
        return face_ref[SLOT[name], k]

    def corner(k, side, part):
        return corner_in[side, k, part]

    mu, dots = ([], {})

    def full_t(j, lo, hi):
        for l in range(layers):
            t = t_ref[j, l, lo:hi]
            for k in range(2):
                if l == ends[k]:
                    t = t - face_ref[SLOT[f"y{j}"], k, lo:hi]
            f_ref[l, lo:hi] = t
            for side in range(2):
                if (0, rows)[side] in (lo, hi):
                    f_ref[l, at[side], :] = f_ref[l, at[side], :] - edge(f"y{j}", side, l)

    def next_v(j, lo, hi):
        for l in order:
            v = local_k(f_ref, l, lo, hi)
            if l in ends:
                v = v + y_ref[j, l, lo:hi]
            v_ref[j + 1, l, lo:hi] = v
            for side in range(2):
                if (0, rows)[side] in (lo, hi):
                    line = y_ref[j, l, at[side], :]
                    v_ref[j + 1, l, at[side], :] = v_ref[j + 1, l, at[side], :] + line

    def next_rows(j, part, sides):
        for l in order:
            for side in sides:
                line = v_ref[j + 1, l, at[side], :] - edge(f"t{j}", side, l)
                for k in range(2):
                    if l == ends[k]:
                        line = line + 2.0 * corner(k, side, part)
                v_ref[j + 1, l, at[side], :] = line

    def next_y(j, which, lo, hi):
        for l in which:
            y_ref[j, l, lo:hi] = m_ref[l, lo:hi] * v_ref[j, l, lo:hi]

    def next_ends(j, lo, hi):
        for k in range(2):
            l = ends[k]
            v = v_ref[j + 1, l, lo:hi] - face_ref[SLOT[f"t{j}"], k, lo:hi]
            v_ref[j + 1, l, lo:hi] = v
            y_ref[j + 1, l, lo:hi] = m_ref[l, lo:hi] * v

    load_k.wait()
    for l in order:
        d = 6.0 + d_ref[l]
        d_ref[l] = d
        m_ref[l] = 1.0 / (d * d + 6.0)
    load_r.wait()
    for l in order:
        y_ref[0, l] = m_ref[l] * v_ref[0, l]
    y, t = y_ref.at[0], t_ref.at[0]
    for side in range(2):
        stage("y0", y, side)
        for k in range(2):
            corner_out[side, k, 0] = y[ends[k], at[side], :]
    pl.semaphore_wait(barrier, greetings)
    for side in range(2):
        edges("y0", y, side)
        corners(side, 0, 1)
    faces("y0", y, 0, 0, cut)
    for l in order:
        t[l] = local_k(y, l)
    faces("t0", t, 0, 0, cut)
    for side in range(2):
        edges("t0", t, side)
    faces("y0", y, 1, cut, rows)
    faces("t0", t, 1, cut, rows)
    mu.append(dot(lambda l: v_ref[0, l], lambda l: y_ref[0, l]))
    dots[0, 0] = dot(lambda l: v_ref[0, l], lambda l: v_ref[0, l])
    y, t = y_ref.at[1], t_ref.at[1]
    spans = [
        [(0, cut), (0, cut_y), (0, cut_t), (0, cut_w)],
        [(cut, rows), (cut_y, rows), (cut_t, rows), (cut_w, rows)],
    ]
    for part in range(2):
        side, (span, span_y, span_t, span_w) = part, spans[part]
        wait_edges("y0", side)
        if part == 0:
            edges("d", d_ref, 0)
            edges("d", d_ref, 1)
            faces("d", d_ref, 0, 0, rows)
        wait_faces("y0", part, *span)
        full_t(0, *span)
        next_v(0, *span_y)
        wait_edges("t0", side)
        wait(corner_in.at[side, :, 0], corner_recv.at[side])
        next_rows(0, 0, (side,))
        next_y(1, inside, *span_y)
        wait_faces("t0", part, *span)
        next_ends(0, *span_y)
        faces("y1", y, part, *span_y)
        edges("y1", y, side)
        for k in range(2):
            corner_out[side, k, OUTER] = y[ends[k], at[side], :]
            corner_out[side, k, INNER_ROW] = y[ends[k], at_second[side], :]
            corner_out[side, k, INNER_LAYER] = y[seconds[k], at[side], :]
        corners(side, OUTER, 3, False)
        lo, hi = span_t
        for l in order:
            t[l, lo:hi] = local_k(y, l, lo, hi)
        faces("t1", t, part, lo, hi)
        edges("t1", t, side)
        for k in range(2):
            corner_out[side, k, PARTIAL] = t[ends[k], at[side], :]
        corners(side, PARTIAL, 1, False)
        lo, hi = span_w
        for l in order:
            w_ref[l, lo:hi] = local_k(t, l, lo, hi)
        faces("w1", w_ref, part, lo, hi)
        edges("w1", w_ref, side)
    mu.append(dot(lambda l: f_ref[l], lambda l: f_ref[l]))
    mu.append(dot(lambda l: v_ref[1, l], lambda l: y_ref[1, l]))
    for i in range(2):
        dots[i, 1] = dot(lambda l: v_ref[i, l], lambda l: v_ref[1, l])
    wait_edges("y1")
    wait_faces("y1")
    full_t(1, 0, rows)
    next_v(1, 0, rows)
    mu.append(dot(lambda l: f_ref[l], lambda l: f_ref[l]))
    wait(edge_in.at[pl.ds(SLOT["d"], 2)], edge_sem("t1", 0))
    wait(corner_in.at[:, :, pl.ds(OUTER, 4)], corner_recv.at[2])
    next_rows(1, OUTER, range(2))
    next_y(2, inside, 0, rows)
    past = {
        (k, side): corner(k, side, PARTIAL) - (edge("y1", side, ends[k]) + face_ref[SLOT["y1"], k, at[side], :])
        for k in range(2)
        for side in range(2)
    }
    edge_part = {}
    for side in range(2):
        lines = []
        for l in range(layers):
            line = y_ref[1, l, at[side], :]
            for k in range(2):
                if l == ends[k]:
                    line = line + corner(k, side, OUTER)
            lines.append(line)
        for l in range(layers):
            beside = across(lines[l])
            if l > 0:
                beside = beside + lines[l - 1]
            if l < layers - 1:
                beside = beside + lines[l + 1]
            part = beside - edge("d", side, l) * lines[l] - f_ref[l, at[side], :]
            for k in range(2):
                if l == ends[k]:
                    part = part + (corner(k, side, INNER_ROW) - past[k, side])
            edge_part[side, l] = part
    wait_faces("d")
    for k in range(2):
        pre_ref[k] = y_ref[1, ends[k]]
        for side in range(2):
            pre_ref[k, at[side], :] = pre_ref[k, at[side], :] + corner(k, side, OUTER)
        a = pre_ref[k]
        d = face("d", k)
        near_m[k] = 1.0 / (d * d + 6.0)
        pre_ref[k] = lateral(a) - d * a - f_ref[ends[k]]
        for side in range(2):
            pre_ref[k, at[side], :] = pre_ref[k, at[side], :] + (corner(k, side, INNER_LAYER) - past[k, side])
    wait_faces("t1")
    next_ends(1, 0, rows)
    y, t = y_ref.at[2], t_ref.at[2]
    for side in range(2):
        for k in range(2):
            corner_out[side, k, LAST] = y[ends[k], at[side], :]
        corners(side, LAST, 1)
    for l in order:
        t[l] = local_k(y, l)
        f_ref[l] = t[l]
    for side in range(2):
        edges("t2", t, side)
    faces("t2", t, 0, 0, rows)
    mu.append(dot(lambda l: v_ref[2, l], lambda l: y_ref[2, l]))
    for i in range(3):
        dots[i, 2] = dot(lambda l: v_ref[i, l], lambda l: v_ref[2, l])
    wait_edges("w1")
    for side in range(2):
        for l in range(layers):
            d = edge("d", side, l)
            y = (edge("w1", side, l) + edge_part[side, l]) / (d * d + 6.0)
            f_ref[l, at[side], :] = f_ref[l, at[side], :] - y
    part = sum(f_ref[l] * f_ref[l] for l in inside)
    line = sums_line(mu, dots, slots.shape[-1])
    wait_faces("w1")
    for k in range(2):
        t = f_ref[ends[k]] - near_m[k] * (face("w1", k) + pre_ref[k])
        f_ref[ends[k]] = t
        part = part + t * t
    mu.append(tile_sum(part))
    lane = lax.broadcasted_iota(jnp.int32, line.shape, 1)
    slots[me] = jnp.where(lane == place(("mu", 2 * ITERS - 1)), mu[-1], line)
    start_sums(slots, sum_send, sum_recv, me, nx, ny)
    next_v(2, 0, rows)
    for side in range(2):
        wait_edges("t2", side)
        wait(corner_in.at[side, :, LAST], corner_recv.at[side])
    next_rows(2, LAST, range(2))
    wait_faces("t2")
    for k in range(2):
        v_ref[3, ends[k]] = v_ref[3, ends[k]] - face("t2", k)

    wait(face_ref, face_send)
    wait(edge_in, edge_send)
    wait(corner_in, corner_send)
    all_slots = slots.at[pl.ds(0, count - 1)]
    pltpu.make_async_copy(all_slots, all_slots, sum_send).wait()
    pltpu.make_async_copy(all_slots, all_slots, sum_recv).wait()
    total = jnp.sum(slots[...], axis=0)

    def whole(name):
        n = place(name)
        return jnp.broadcast_to(total[:, n : n + 1], total.shape)

    mu = [whole(("mu", i)) for i in range(2 * ITERS)]
    got = {name: whole(name) for name in dots}
    sol, res, norms = coefficients(mu, got, float(cells))
    for k, value in enumerate(norms + sol[:ITERS] + res[1:]):
        coef_ref[k] = value


def place(name):
    names = [("mu", i) for i in range(2 * ITERS)]
    names += [(i, j) for j in range(ITERS) for i in range(j + 1)]
    return names.index(name)


def sums_line(mu, dots, size):
    lane = lax.broadcasted_iota(jnp.int32, (1, size), 1)
    line = jnp.zeros(lane.shape, jnp.float32)
    named = [(("mu", i), value) for i, value in enumerate(mu)] + list(dots.items())
    for name, value in named:
        line = jnp.where(lane == place(name), value, line)
    return line


def start_sums(slots, sum_send, sum_recv, me, nx, ny):
    def send(x, y):
        pltpu.make_async_remote_copy(
            src_ref=slots.at[me],
            dst_ref=slots.at[me],
            send_sem=sum_send,
            recv_sem=sum_recv,
            device_id=(x, y),
            device_id_type=MESH,
        ).start()

    ix, iy = lax.axis_index("gx"), lax.axis_index("gy")
    for k in range(ny - 1):
        send(ix, jnp.where(iy <= k, k + 1, k))

    def send_line(k, carry):
        x = jnp.where(ix <= k, k + 1, k)
        for y in range(ny):
            send(x, y)
        return carry

    lax.fori_loop(0, nx - 1, send_line, 0, unroll=nx * ny <= 64)


def finish(coef, v_ref, y_ref, sol_ref, res_ref, norms_ref):
    cols = v_ref.shape[-1]
    lines = [jnp.concatenate([coef[k]] * (cols // coef.shape[-1]), axis=1) for k in range(3 * ITERS)]
    for l in range(v_ref.shape[1]):
        sol = lines[ITERS] * y_ref[0, l]
        res = v_ref[0, l]
        for i in range(1, ITERS):
            sol = sol + lines[ITERS + i] * y_ref[i, l]
        for i in range(1, ITERS + 1):
            res = res + lines[2 * ITERS + i - 1] * v_ref[i, l]
        sol_ref[l] = sol
        res_ref[l] = res
    lane = lax.broadcasted_iota(jnp.int32, coef.shape[1:], 1)
    line = coef[0]
    for i in range(1, ITERS):
        line = jnp.where(lane == i, coef[i], line)
    norms_ref[...] = line[0, :ITERS]


def body(right_side, kappa_sq):
    nx, ny = lax.axis_size("gx"), lax.axis_size("gy")
    shape = right_side.shape
    layers, rows, cols = shape
    cells = nx * layers * ny * rows * cols
    f32 = jnp.float32
    dma = pltpu.SemaphoreType.DMA
    whole = pl.BlockSpec(memory_space=pltpu.VMEM)
    out = pl.pallas_call(
        functools.partial(kernel, nx, ny, cells),
        out_shape=(
            pltpu.VMEM((ITERS + 1,) + shape, f32),
            pltpu.VMEM((ITERS,) + shape, f32),
            pltpu.VMEM((3 * ITERS, 1, 128), f32),
        ),
        in_specs=[pl.BlockSpec(memory_space=pl.ANY)] * 2,
        out_specs=(whole, whole, whole),
        scratch_shapes=[
            pltpu.VMEM((ITERS,) + shape, f32),
            pltpu.VMEM(shape, f32),
            pltpu.VMEM(shape, f32),
            pltpu.VMEM(shape, f32),
            pltpu.VMEM(shape, f32),
            pltpu.VMEM((2, rows, cols), f32),
            pltpu.VMEM((2, rows, cols), f32),
            pltpu.VMEM((len(FACES), 2, rows, cols), f32),
            pltpu.VMEM((len(FACES), 2, layers, 1, cols), f32),
            pltpu.VMEM((len(FACES), 2, layers, 1, cols), f32),
            pltpu.VMEM((2, 2, 6, 1, cols), f32),
            pltpu.VMEM((2, 2, 6, 1, cols), f32),
            pltpu.VMEM((nx * ny, 1, 128), f32),
            dma((2,)),
            dma((len(ARRIVALS),)),
            dma(()),
            dma((len(ARRIVALS) - 1,)),
            dma((3,)),
            dma(()),
            dma(()),
        ],
        compiler_params=pltpu.CompilerParams(collective_id=0, has_side_effects=True),
    )(right_side, kappa_sq)
    return pl.pallas_call(
        finish,
        out_shape=(
            jax.ShapeDtypeStruct(shape, f32),
            jax.ShapeDtypeStruct(shape, f32),
            jax.ShapeDtypeStruct((ITERS,), f32),
        ),
        in_specs=[whole, whole, whole],
        out_specs=(whole, whole, whole),
    )(*(pltpu.with_memory_space_constraint(x, pltpu.VMEM) for x in (out[2], out[0], out[1])))


def solution(mesh):
    return jax.shard_map(
        body,
        mesh=mesh,
        in_specs=(P("gx", "gy", None), P("gx", "gy", None)),
        out_specs=(P("gx", "gy", None), P("gx", "gy", None), P()),
        check_vma=False,
    )
```

```python
import functools
import jax
import jax.numpy as jnp
from jax import lax
from jax.experimental import pallas as pl
from jax.experimental.pallas import tpu as pltpu
from jax.sharding import PartitionSpec as P

ITERS = 3
MESH = pl.DeviceIdType.MESH


def shifted(c):
    return [None] + c[:-1]


def plus(a, b, scale):
    out = []
    for one, two in zip(a, b):
        two = None if two is None else two * scale
        out.append(one if two is None else two if one is None else one + two)
    return out


def form(c, entry):
    total = None
    for i, one in enumerate(c):
        for j, two in enumerate(c):
            if one is not None and two is not None and i < ITERS and j < ITERS:
                term = one * two * entry(i, j)
                total = term if total is None else total + term
    return total


def coefficients(mu, dots, cells):
    one = jnp.ones_like(mu[0])
    res = [one] + [None] * ITERS
    step = [None] * (ITERS + 1)
    sol = [None] * (ITERS + 1)
    norms = []
    for i in range(ITERS):
        gamma = form(res, lambda a, b: mu[a + b])
        delta = form(res, lambda a, b: mu[a + b + 1])
        norms.append(jnp.sqrt(form(res, lambda a, b: dots[min(a, b), max(a, b)]) / cells))
        if i == 0:
            alpha = gamma / delta
            step = list(res)
        else:
            beta = gamma / gamma_old
            alpha = gamma / (delta - beta * gamma / alpha_old)
            step = plus(res, step, beta)
        sol = plus(sol, step, alpha)
        res = plus(res, shifted(step), -alpha)
        gamma_old, alpha_old = gamma, alpha
    return sol, res, norms


FACES = ("y0", "t0", "y1", "d", "t1", "w1", "t2")
SLOT = {name: i for i, name in enumerate(FACES)}
SAME = {"t2": "y0"}
SPLIT = ("y0", "t0")
ARRIVALS = tuple((name, part) for name in SPLIT for part in range(2)) + tuple(
    (name, 0) for name in ("y1", "t1", "w1", "d")
)
TILE = 8
OUTER, INNER_ROW, INNER_LAYER, PARTIAL, LAST = 1, 2, 3, 4, 5


def kernel(
    nx, ny, cells, rhs_hbm, kappa_hbm, *refs,
):
    (
    v_ref, y_ref, coef_ref, t_ref, f_ref, w_ref, d_ref, m_ref, pre_ref, near_m, face_ref, edge_out, edge_in,
    corner_out, corner_in, slots, load_sem, face_recv, edge_send, edge_recv,
    corner_recv, sum_send, sum_recv,
    ) = refs
    layers, rows, cols = rhs_hbm.shape
    assert layers >= 3 and rows % TILE == 0 and rows >= 6 * TILE
    cut_w = rows // (4 * TILE) * TILE
    cut_t, cut_y, cut = cut_w + TILE, cut_w + 2 * TILE, cut_w + 3 * TILE
    ix, iy = lax.axis_index("gx"), lax.axis_index("gy")
    count = nx * ny
    me = ix * ny + iy
    ends, seconds = (0, layers - 1), (1, layers - 2)
    order = [0, layers - 1] + list(range(1, layers - 1))
    inside = list(range(1, layers - 1))
    face_send, corner_send = load_sem.at[0], load_sem.at[1]
    load_k = pltpu.make_async_copy(kappa_hbm, d_ref, load_sem.at[0])
    load_r = pltpu.make_async_copy(rhs_hbm, v_ref.at[0], load_sem.at[1])
    load_k.start()
    load_r.start()

    barrier = pltpu.get_barrier_semaphore()
    x_of = (lax.rem(ix + nx - 1, nx), lax.rem(ix + 1, nx))
    y_of = (lax.rem(iy + ny - 1, ny), lax.rem(iy + 1, ny))

    near = ny // 2 <= 2

    def greet(x, y):
        pl.semaphore_signal(barrier, inc=1, device_id=(x, y), device_id_type=MESH)

    def greet_any(k, carry):
        other = lax.rem(me + k, count)
        greet(other // ny, lax.rem(other, ny))
        return carry

    def greet_x(k, carry):
        greet(lax.rem(ix + k, nx), iy)
        return carry

    def greet_y(k, carry):
        greet(ix, lax.rem(iy + k, ny))
        return carry

    if near:
        for x in x_of:
            greet(x, iy)
        for y in y_of:
            for x in x_of:
                greet(x, y)
        lax.fori_loop(1, ny, greet_y, 0)
        lax.fori_loop(2, nx - 1, greet_x, 0)
        greetings = nx - 1 + ny - 1 + 4
    else:
        lax.fori_loop(1, count, greet_any, 0)
        greetings = count - 1

    row = lax.broadcasted_iota(jnp.int32, (rows, cols), 0)
    first, last = row == 0, row == rows - 1

    def across(x):
        return pltpu.roll(x, 1, 1) + pltpu.roll(x, cols - 1, 1)

    def lateral(x):
        up = jnp.where(first, 0.0, pltpu.roll(x, 1, 0))
        down = jnp.where(last, 0.0, pltpu.roll(x, rows - 1, 0))
        return across(x) + (up + down)

    def local_k(ref, l, lo=0, hi=rows):
        a, b = max(lo - TILE, 0), min(hi + TILE, rows)
        x = ref[l, a:b]
        up, down = pltpu.roll(x, 1, 0), pltpu.roll(x, b - a - 1, 0)
        if a == 0:
            up = jnp.where(row[: b - a] == 0, 0.0, up)
        if b == rows:
            down = jnp.where(row[: b - a] == b - a - 1, 0.0, down)
        mid = slice(lo - a, hi - a)
        x = x[mid]
        out = d_ref[l, lo:hi] * x - (across(x) + (up[mid] + down[mid]))
        if l > 0:
            out = out - ref[l - 1, lo:hi]
        if l < layers - 1:
            out = out - ref[l + 1, lo:hi]
        return out

    def tile_sum(x):
        return jnp.sum(x, axis=(0, 1), keepdims=True)

    def dot(a, b):
        return tile_sum(sum(a(l) * b(l) for l in range(layers)))

    at = [pl.ds((0, rows - 1)[side], 1) for side in range(2)]
    at_second = [pl.ds((1, rows - 2)[side], 1) for side in range(2)]
    def remote(src, dst, send, recv, device):
        pltpu.make_async_remote_copy(
            src_ref=src, dst_ref=dst, send_sem=send, recv_sem=recv,
            device_id=device, device_id_type=MESH,
        ).start()

    def wait(ref, sem):
        pltpu.make_async_copy(ref, ref, sem).wait()

    def edge_sem(name, side):
        first = name in SPLIT
        return edge_recv.at[side if first else ARRIVALS.index((name, 0)) - 2]

    def stage(name, src, side):
        for l in range(layers):
            edge_out[SLOT[name], side, l] = src[l, at[side], :]

    def edges(name, src, side):
        n = SLOT[name]
        if name not in SPLIT + ("d",):
            stage(name, src, side)
        sem = edge_sem("t1" if name == "d" else SAME.get(name, name), 1 - side)
        remote(edge_out.at[n, side], edge_in.at[n, 1 - side], edge_send, sem, (ix, y_of[side]))

    def wait_edges(name, side=None):
        if side is None:
            wait(edge_in.at[SLOT[name]], edge_sem(name, 0))
        else:
            wait(edge_in.at[SLOT[name], side], edge_sem(SAME.get(name, name), side))

    def face_sem(name, part):
        return face_recv.at[ARRIVALS.index((name, part if name in SPLIT else 0))]

    def faces(name, src, part, lo, hi):
        n, span = SLOT[name], pl.ds(lo, hi - lo)
        sem = face_sem(SAME.get(name, name), part)
        for k in range(2):
            remote(
                src.at[ends[k], span], face_ref.at[n, 1 - k, span], face_send, sem, (x_of[k], iy)
            )

    def wait_faces(name, part=0, lo=0, hi=rows):
        sem = face_sem(SAME.get(name, name), part)
        wait(face_ref.at[SLOT[name], :, pl.ds(lo, hi - lo)], sem)

    def corners(side, start, size, again=True):
        sem = corner_recv.at[1 - side if again else 2]
        for k in range(2):
            span = pl.ds(start, size)
            remote(
                corner_out.at[side, k, span], corner_in.at[1 - side, 1 - k, span],
                corner_send, sem, (x_of[k], y_of[side]),
            )

    def edge(name, side, l):
        return edge_in[SLOT[name], side, l]

    def face(name, k):
        return face_ref[SLOT[name], k]

    def corner(k, side, part):
        return corner_in[side, k, part]

    mu, dots = ([], {})

    def full_t(j, lo, hi):
        for l in range(layers):
            t = t_ref[j, l, lo:hi]
            for k in range(2):
                if l == ends[k]:
                    t = t - face_ref[SLOT[f"y{j}"], k, lo:hi]
            f_ref[l, lo:hi] = t
            for side in range(2):
                if (0, rows)[side] in (lo, hi):
                    f_ref[l, at[side], :] = f_ref[l, at[side], :] - edge(f"y{j}", side, l)

    def next_v(j, lo, hi):
        for l in order:
            v = local_k(f_ref, l, lo, hi)
            if l in ends:
                v = v + y_ref[j, l, lo:hi]
            v_ref[j + 1, l, lo:hi] = v
            for side in range(2):
                if (0, rows)[side] in (lo, hi):
                    line = y_ref[j, l, at[side], :]
                    v_ref[j + 1, l, at[side], :] = v_ref[j + 1, l, at[side], :] + line

    def next_rows(j, part, sides):
        for l in order:
            for side in sides:
                line = v_ref[j + 1, l, at[side], :] - edge(f"t{j}", side, l)
                for k in range(2):
                    if l == ends[k]:
                        line = line + 2.0 * corner(k, side, part)
                v_ref[j + 1, l, at[side], :] = line

    def next_y(j, which, lo, hi):
        for l in which:
            y_ref[j, l, lo:hi] = m_ref[l, lo:hi] * v_ref[j, l, lo:hi]

    def next_ends(j, lo, hi):
        for k in range(2):
            l = ends[k]
            v = v_ref[j + 1, l, lo:hi] - face_ref[SLOT[f"t{j}"], k, lo:hi]
            v_ref[j + 1, l, lo:hi] = v
            y_ref[j + 1, l, lo:hi] = m_ref[l, lo:hi] * v

    load_k.wait()
    for l in order:
        d = 6.0 + d_ref[l]
        d_ref[l] = d
        m_ref[l] = 1.0 / (d * d + 6.0)
    load_r.wait()
    for l in order:
        y_ref[0, l] = m_ref[l] * v_ref[0, l]
    y, t = y_ref.at[0], t_ref.at[0]
    for side in range(2):
        stage("y0", y, side)
        stage("d", d_ref, side)
        for k in range(2):
            corner_out[side, k, 0] = y[ends[k], at[side], :]
    for l in order:
        t[l] = local_k(y, l)
    for side in range(2):
        stage("t0", t, side)
    pl.semaphore_wait(barrier, greetings)
    for side in range(2):
        corners(side, 0, 1)
    faces("y0", y, 0, 0, cut)
    for side in range(2):
        edges("y0", y, side)
    faces("t0", t, 0, 0, cut)
    for side in range(2):
        edges("t0", t, side)
    faces("y0", y, 1, cut, rows)
    faces("t0", t, 1, cut, rows)
    for side in range(2):
        edges("d", d_ref, side)
    mu.append(dot(lambda l: v_ref[0, l], lambda l: y_ref[0, l]))
    dots[0, 0] = dot(lambda l: v_ref[0, l], lambda l: v_ref[0, l])
    y, t = y_ref.at[1], t_ref.at[1]
    spans = [
        [(0, cut), (0, cut_y), (0, cut_t), (0, cut_w)],
        [(cut, rows), (cut_y, rows), (cut_t, rows), (cut_w, rows)],
    ]
    for part in range(2):
        side, (span, span_y, span_t, span_w) = part, spans[part]
        wait(edge_in.at[pl.ds(SLOT["y0"], 2), side], edge_sem("y0", side))
        if part == 0:
            faces("d", d_ref, 0, 0, rows)
        wait_faces("y0", part, *span)
        full_t(0, *span)
        next_v(0, *span_y)
        wait(corner_in.at[side, :, 0], corner_recv.at[side])
        next_rows(0, 0, (side,))
        next_y(1, inside, *span_y)
        wait_faces("t0", part, *span)
        next_ends(0, *span_y)
        faces("y1", y, part, *span_y)
        edges("y1", y, side)
        for k in range(2):
            corner_out[side, k, OUTER] = y[ends[k], at[side], :]
            corner_out[side, k, INNER_ROW] = y[ends[k], at_second[side], :]
            corner_out[side, k, INNER_LAYER] = y[seconds[k], at[side], :]
        corners(side, OUTER, 3, False)
        lo, hi = span_t
        for l in order:
            t[l, lo:hi] = local_k(y, l, lo, hi)
        faces("t1", t, part, lo, hi)
        edges("t1", t, side)
        for k in range(2):
            corner_out[side, k, PARTIAL] = t[ends[k], at[side], :]
        corners(side, PARTIAL, 1, False)
        lo, hi = span_w
        for l in order:
            w_ref[l, lo:hi] = local_k(t, l, lo, hi)
        faces("w1", w_ref, part, lo, hi)
        edges("w1", w_ref, side)
    mu.append(dot(lambda l: f_ref[l], lambda l: f_ref[l]))
    mu.append(dot(lambda l: v_ref[1, l], lambda l: y_ref[1, l]))
    for i in range(2):
        dots[i, 1] = dot(lambda l: v_ref[i, l], lambda l: v_ref[1, l])
    wait_edges("y1")
    wait_faces("y1")
    full_t(1, 0, rows)
    next_v(1, 0, rows)
    mu.append(dot(lambda l: f_ref[l], lambda l: f_ref[l]))
    wait(edge_in.at[pl.ds(SLOT["d"], 2)], edge_sem("t1", 0))
    wait(corner_in.at[:, :, pl.ds(OUTER, 4)], corner_recv.at[2])
    next_rows(1, OUTER, range(2))
    next_y(2, inside, 0, rows)
    past = {
        (k, side): corner(k, side, PARTIAL) - (edge("y1", side, ends[k]) + face_ref[SLOT["y1"], k, at[side], :])
        for k in range(2)
        for side in range(2)
    }
    edge_part = {}
    for side in range(2):
        lines = []
        for l in range(layers):
            line = y_ref[1, l, at[side], :]
            for k in range(2):
                if l == ends[k]:
                    line = line + corner(k, side, OUTER)
            lines.append(line)
        for l in range(layers):
            beside = across(lines[l])
            if l > 0:
                beside = beside + lines[l - 1]
            if l < layers - 1:
                beside = beside + lines[l + 1]
            part = beside - edge("d", side, l) * lines[l] - f_ref[l, at[side], :]
            for k in range(2):
                if l == ends[k]:
                    part = part + (corner(k, side, INNER_ROW) - past[k, side])
            edge_part[side, l] = part
    wait_faces("d")
    for k in range(2):
        pre_ref[k] = y_ref[1, ends[k]]
        for side in range(2):
            pre_ref[k, at[side], :] = pre_ref[k, at[side], :] + corner(k, side, OUTER)
        a = pre_ref[k]
        d = face("d", k)
        near_m[k] = 1.0 / (d * d + 6.0)
        pre_ref[k] = lateral(a) - d * a - f_ref[ends[k]]
        for side in range(2):
            pre_ref[k, at[side], :] = pre_ref[k, at[side], :] + (corner(k, side, INNER_LAYER) - past[k, side])
    wait_faces("t1")
    next_ends(1, 0, rows)
    y, t = y_ref.at[2], t_ref.at[2]
    for side in range(2):
        for k in range(2):
            corner_out[side, k, LAST] = y[ends[k], at[side], :]
        corners(side, LAST, 1)
    for l in order:
        t[l] = local_k(y, l)
        f_ref[l] = t[l]
    for side in range(2):
        edges("t2", t, side)
    faces("t2", t, 0, 0, rows)
    mu.append(dot(lambda l: v_ref[2, l], lambda l: y_ref[2, l]))
    for i in range(3):
        dots[i, 2] = dot(lambda l: v_ref[i, l], lambda l: v_ref[2, l])
    wait_edges("w1")
    for side in range(2):
        for l in range(layers):
            d = edge("d", side, l)
            y = (edge("w1", side, l) + edge_part[side, l]) / (d * d + 6.0)
            f_ref[l, at[side], :] = f_ref[l, at[side], :] - y
    part = sum(f_ref[l] * f_ref[l] for l in inside)
    line = sums_line(mu, dots, slots.shape[-1])
    wait_faces("w1")
    for k in range(2):
        t = f_ref[ends[k]] - near_m[k] * (face("w1", k) + pre_ref[k])
        part = part + t * t
    mu.append(tile_sum(part))
    lane = lax.broadcasted_iota(jnp.int32, line.shape, 1)
    slots[me] = jnp.where(lane == place(("mu", 2 * ITERS - 1)), mu[-1], line)
    start_sums(slots, sum_send, sum_recv, me, nx, ny)
    for k in range(2):
        f_ref[ends[k]] = f_ref[ends[k]] - near_m[k] * (face("w1", k) + pre_ref[k])
    next_v(2, 0, rows)
    for side in range(2):
        wait_edges("t2", side)
        wait(corner_in.at[side, :, LAST], corner_recv.at[side])
    next_rows(2, LAST, range(2))
    wait_faces("t2")
    for k in range(2):
        v_ref[3, ends[k]] = v_ref[3, ends[k]] - face("t2", k)

    wait(face_ref, face_send)
    wait(edge_in, edge_send)
    wait(corner_in, corner_send)
    all_slots = slots.at[pl.ds(0, count - 1)]
    pltpu.make_async_copy(all_slots, all_slots, sum_send).wait()
    pltpu.make_async_copy(all_slots, all_slots, sum_recv).wait()
    total = jnp.sum(slots[...], axis=0)

    def whole(name):
        n = place(name)
        return jnp.broadcast_to(total[:, n : n + 1], total.shape)

    mu = [whole(("mu", i)) for i in range(2 * ITERS)]
    got = {name: whole(name) for name in dots}
    sol, res, norms = coefficients(mu, got, float(cells))
    for k, value in enumerate(norms + sol[:ITERS] + res[1:]):
        coef_ref[k] = value


def place(name):
    names = [("mu", i) for i in range(2 * ITERS)]
    names += [(i, j) for j in range(ITERS) for i in range(j + 1)]
    return names.index(name)


def sums_line(mu, dots, size):
    lane = lax.broadcasted_iota(jnp.int32, (1, size), 1)
    line = jnp.zeros(lane.shape, jnp.float32)
    named = [(("mu", i), value) for i, value in enumerate(mu)] + list(dots.items())
    for name, value in named:
        line = jnp.where(lane == place(name), value, line)
    return line


def start_sums(slots, sum_send, sum_recv, me, nx, ny):
    def send(x, y):
        pltpu.make_async_remote_copy(
            src_ref=slots.at[me],
            dst_ref=slots.at[me],
            send_sem=sum_send,
            recv_sem=sum_recv,
            device_id=(x, y),
            device_id_type=MESH,
        ).start()

    ix, iy = lax.axis_index("gx"), lax.axis_index("gy")
    for k in range(ny - 1):
        send(ix, jnp.where(iy <= k, k + 1, k))

    def send_line(k, carry):
        x = jnp.where(ix <= k, k + 1, k)
        for y in range(ny):
            send(x, y)
        return carry

    lax.fori_loop(0, nx - 1, send_line, 0, unroll=nx * ny <= 64)


def finish(coef, v_ref, y_ref, sol_ref, res_ref, norms_ref):
    cols = v_ref.shape[-1]
    lines = [jnp.concatenate([coef[k]] * (cols // coef.shape[-1]), axis=1) for k in range(3 * ITERS)]
    half = v_ref.shape[1] // pl.num_programs(0)
    for n in range(half):
        l = pl.program_id(0) * half + n
        sol = lines[ITERS] * y_ref[0, l]
        res = v_ref[0, l]
        for i in range(1, ITERS):
            sol = sol + lines[ITERS + i] * y_ref[i, l]
        for i in range(1, ITERS + 1):
            res = res + lines[2 * ITERS + i - 1] * v_ref[i, l]
        sol_ref[n] = sol
        res_ref[n] = res
    lane = lax.broadcasted_iota(jnp.int32, coef.shape[1:], 1)
    line = coef[0]
    for i in range(1, ITERS):
        line = jnp.where(lane == i, coef[i], line)
    norms_ref[...] = line[0, :ITERS]


def body(right_side, kappa_sq):
    nx, ny = lax.axis_size("gx"), lax.axis_size("gy")
    shape = right_side.shape
    layers, rows, cols = shape
    cells = nx * layers * ny * rows * cols
    f32 = jnp.float32
    dma = pltpu.SemaphoreType.DMA
    whole = pl.BlockSpec(memory_space=pltpu.VMEM)
    out = pl.pallas_call(
        functools.partial(kernel, nx, ny, cells),
        out_shape=(
            pltpu.VMEM((ITERS + 1,) + shape, f32),
            pltpu.VMEM((ITERS,) + shape, f32),
            pltpu.VMEM((3 * ITERS, 1, 128), f32),
        ),
        in_specs=[pl.BlockSpec(memory_space=pl.ANY)] * 2,
        out_specs=(whole, whole, whole),
        scratch_shapes=[
            pltpu.VMEM((ITERS,) + shape, f32),
            pltpu.VMEM(shape, f32),
            pltpu.VMEM(shape, f32),
            pltpu.VMEM(shape, f32),
            pltpu.VMEM(shape, f32),
            pltpu.VMEM((2, rows, cols), f32),
            pltpu.VMEM((2, rows, cols), f32),
            pltpu.VMEM((len(FACES), 2, rows, cols), f32),
            pltpu.VMEM((len(FACES), 2, layers, 1, cols), f32),
            pltpu.VMEM((len(FACES), 2, layers, 1, cols), f32),
            pltpu.VMEM((2, 2, 6, 1, cols), f32),
            pltpu.VMEM((2, 2, 6, 1, cols), f32),
            pltpu.VMEM((nx * ny, 1, 128), f32),
            dma((2,)),
            dma((len(ARRIVALS),)),
            dma(()),
            dma((len(ARRIVALS) - 3,)),
            dma((3,)),
            dma(()),
            dma(()),
        ],
        compiler_params=pltpu.CompilerParams(collective_id=0, has_side_effects=True),
    )(right_side, kappa_sq)
    return pl.pallas_call(
        finish,
        out_shape=(
            jax.ShapeDtypeStruct(shape, f32),
            jax.ShapeDtypeStruct(shape, f32),
            jax.ShapeDtypeStruct((ITERS,), f32),
        ),
        grid=(2,),
        in_specs=[whole, whole, whole],
        out_specs=(pl.BlockSpec((layers // 2, rows, cols), lambda h: (h, 0, 0)),) * 2 + (whole,),
    )(*(pltpu.with_memory_space_constraint(x, pltpu.VMEM) for x in (out[2], out[0], out[1])))


def solution(mesh):
    return jax.shard_map(
        body,
        mesh=mesh,
        in_specs=(P("gx", "gy", None), P("gx", "gy", None)),
        out_specs=(P("gx", "gy", None), P("gx", "gy", None), P()),
        check_vma=False,
    )
```

```python
import functools
import jax
import jax.numpy as jnp
from jax import lax
from jax.experimental import pallas as pl
from jax.experimental.pallas import tpu as pltpu
from jax.sharding import PartitionSpec as P

ITERS = 3
MESH = pl.DeviceIdType.MESH


def shifted(c):
    return [None] + c[:-1]


def plus(a, b, scale):
    out = []
    for one, two in zip(a, b):
        two = None if two is None else two * scale
        out.append(one if two is None else two if one is None else one + two)
    return out


def form(c, entry):
    total = None
    for i, one in enumerate(c):
        for j, two in enumerate(c):
            if one is not None and two is not None and i < ITERS and j < ITERS:
                term = one * two * entry(i, j)
                total = term if total is None else total + term
    return total


def coefficients(mu, dots, cells):
    one = jnp.ones_like(mu[0])
    res = [one] + [None] * ITERS
    step = [None] * (ITERS + 1)
    sol = [None] * (ITERS + 1)
    norms = []
    for i in range(ITERS):
        gamma = form(res, lambda a, b: mu[a + b])
        delta = form(res, lambda a, b: mu[a + b + 1])
        norms.append(jnp.sqrt(form(res, lambda a, b: dots[min(a, b), max(a, b)]) / cells))
        if i == 0:
            alpha = gamma / delta
            step = list(res)
        else:
            beta = gamma / gamma_old
            alpha = gamma / (delta - beta * gamma / alpha_old)
            step = plus(res, step, beta)
        sol = plus(sol, step, alpha)
        res = plus(res, shifted(step), -alpha)
        gamma_old, alpha_old = gamma, alpha
    return sol, res, norms


FACES = ("y0", "t0", "y1", "d", "t1", "w1", "t2")
SLOT = {name: i for i, name in enumerate(FACES)}
SAME = {"t2": "y0"}
SPLIT = ("y0", "t0")
ARRIVALS = tuple((name, part) for name in SPLIT for part in range(2)) + tuple(
    (name, 0) for name in ("y1", "t1", "w1", "d")
)
TILE = 8
OUTER, INNER_ROW, INNER_LAYER, PARTIAL, LAST = 1, 2, 3, 4, 5


def kernel(
    nx, ny, cells, rhs_hbm, kappa_hbm, *refs,
):
    (
    v_ref, y_ref, coef_ref, t_ref, f_ref, w_ref, d_ref, m_ref, pre_ref, near_m, face_ref, edge_out, edge_in,
    corner_out, corner_in, slots, load_sem, face_recv, edge_send, edge_recv,
    corner_recv, sum_send, sum_recv,
    ) = refs
    layers, rows, cols = rhs_hbm.shape
    assert layers >= 3 and rows % TILE == 0 and rows >= 6 * TILE
    cut_w = rows // (4 * TILE) * TILE
    cut_t, cut_y, cut = cut_w + TILE, cut_w + 2 * TILE, cut_w + 3 * TILE
    ix, iy = lax.axis_index("gx"), lax.axis_index("gy")
    count = nx * ny
    me = ix * ny + iy
    ends, seconds = (0, layers - 1), (1, layers - 2)
    order = [0, layers - 1] + list(range(1, layers - 1))
    inside = list(range(1, layers - 1))
    face_send, corner_send = load_sem.at[0], load_sem.at[1]
    load_k = pltpu.make_async_copy(kappa_hbm, d_ref, load_sem.at[0])
    load_r = pltpu.make_async_copy(rhs_hbm, v_ref.at[0], load_sem.at[1])

    barrier = pltpu.get_barrier_semaphore()
    x_of = (lax.rem(ix + nx - 1, nx), lax.rem(ix + 1, nx))
    y_of = (lax.rem(iy + ny - 1, ny), lax.rem(iy + 1, ny))

    near = ny // 2 <= 2

    def greet(x, y):
        pl.semaphore_signal(barrier, inc=1, device_id=(x, y), device_id_type=MESH)

    def greet_any(k, carry):
        other = lax.rem(me + k, count)
        greet(other // ny, lax.rem(other, ny))
        return carry

    def greet_x(k, carry):
        greet(lax.rem(ix + k, nx), iy)
        return carry

    def greet_y(k, carry):
        greet(ix, lax.rem(iy + k, ny))
        return carry

    if near:
        for x in x_of:
            greet(x, iy)
        load_k.start()
        load_r.start()
        for y in y_of:
            for x in x_of:
                greet(x, y)
        lax.fori_loop(1, ny, greet_y, 0)
        lax.fori_loop(2, nx - 1, greet_x, 0)
        greetings = nx - 1 + ny - 1 + 4
    else:
        load_k.start()
        load_r.start()
        lax.fori_loop(1, count, greet_any, 0)
        greetings = count - 1

    row = lax.broadcasted_iota(jnp.int32, (rows, cols), 0)
    first, last = row == 0, row == rows - 1

    def across(x):
        return pltpu.roll(x, 1, 1) + pltpu.roll(x, cols - 1, 1)

    def lateral(x):
        up = jnp.where(first, 0.0, pltpu.roll(x, 1, 0))
        down = jnp.where(last, 0.0, pltpu.roll(x, rows - 1, 0))
        return across(x) + (up + down)

    def local_k(ref, l, lo=0, hi=rows):
        a, b = max(lo - TILE, 0), min(hi + TILE, rows)
        x = ref[l, a:b]
        up, down = pltpu.roll(x, 1, 0), pltpu.roll(x, b - a - 1, 0)
        if a == 0:
            up = jnp.where(row[: b - a] == 0, 0.0, up)
        if b == rows:
            down = jnp.where(row[: b - a] == b - a - 1, 0.0, down)
        mid = slice(lo - a, hi - a)
        x = x[mid]
        out = d_ref[l, lo:hi] * x - (across(x) + (up[mid] + down[mid]))
        if l > 0:
            out = out - ref[l - 1, lo:hi]
        if l < layers - 1:
            out = out - ref[l + 1, lo:hi]
        return out

    def tile_sum(x):
        return jnp.sum(x, axis=(0, 1), keepdims=True)

    def dot(a, b):
        return tile_sum(sum(a(l) * b(l) for l in range(layers)))

    at = [pl.ds((0, rows - 1)[side], 1) for side in range(2)]
    at_second = [pl.ds((1, rows - 2)[side], 1) for side in range(2)]
    def remote(src, dst, send, recv, device):
        pltpu.make_async_remote_copy(
            src_ref=src, dst_ref=dst, send_sem=send, recv_sem=recv,
            device_id=device, device_id_type=MESH,
        ).start()

    def wait(ref, sem):
        pltpu.make_async_copy(ref, ref, sem).wait()

    def edge_sem(name, side):
        first = name in SPLIT
        return edge_recv.at[side if first else ARRIVALS.index((name, 0)) - 2]

    def stage(name, src, side):
        for l in range(layers):
            edge_out[SLOT[name], side, l] = src[l, at[side], :]

    def edges(name, src, side):
        n = SLOT[name]
        if name not in SPLIT + ("d",):
            stage(name, src, side)
        sem = edge_sem("t1" if name == "d" else SAME.get(name, name), 1 - side)
        remote(edge_out.at[n, side], edge_in.at[n, 1 - side], edge_send, sem, (ix, y_of[side]))

    def wait_edges(name, side=None):
        if side is None:
            wait(edge_in.at[SLOT[name]], edge_sem(name, 0))
        else:
            wait(edge_in.at[SLOT[name], side], edge_sem(SAME.get(name, name), side))

    def face_sem(name, part):
        return face_recv.at[ARRIVALS.index((name, part if name in SPLIT else 0))]

    def faces(name, src, part, lo, hi):
        n, span = SLOT[name], pl.ds(lo, hi - lo)
        sem = face_sem(SAME.get(name, name), part)
        for k in range(2):
            remote(
                src.at[ends[k], span], face_ref.at[n, 1 - k, span], face_send, sem, (x_of[k], iy)
            )

    def wait_faces(name, part=0, lo=0, hi=rows):
        sem = face_sem(SAME.get(name, name), part)
        wait(face_ref.at[SLOT[name], :, pl.ds(lo, hi - lo)], sem)

    def corners(side, start, size, again=True):
        sem = corner_recv.at[1 - side if again else 2]
        for k in range(2):
            span = pl.ds(start, size)
            remote(
                corner_out.at[side, k, span], corner_in.at[1 - side, 1 - k, span],
                corner_send, sem, (x_of[k], y_of[side]),
            )

    def edge(name, side, l):
        return edge_in[SLOT[name], side, l]

    def face(name, k):
        return face_ref[SLOT[name], k]

    def corner(k, side, part):
        return corner_in[side, k, part]

    mu, dots = ([], {})

    def full_t(j, lo, hi):
        for l in range(layers):
            t = t_ref[j, l, lo:hi]
            for k in range(2):
                if l == ends[k]:
                    t = t - face_ref[SLOT[f"y{j}"], k, lo:hi]
            f_ref[l, lo:hi] = t
            for side in range(2):
                if (0, rows)[side] in (lo, hi):
                    f_ref[l, at[side], :] = f_ref[l, at[side], :] - edge(f"y{j}", side, l)

    def next_v(j, lo, hi):
        for l in order:
            v = local_k(f_ref, l, lo, hi)
            if l in ends:
                v = v + y_ref[j, l, lo:hi]
            v_ref[j + 1, l, lo:hi] = v
            for side in range(2):
                if (0, rows)[side] in (lo, hi):
                    line = y_ref[j, l, at[side], :]
                    v_ref[j + 1, l, at[side], :] = v_ref[j + 1, l, at[side], :] + line

    def next_rows(j, part, sides):
        for l in order:
            for side in sides:
                line = v_ref[j + 1, l, at[side], :] - edge(f"t{j}", side, l)
                for k in range(2):
                    if l == ends[k]:
                        line = line + 2.0 * corner(k, side, part)
                v_ref[j + 1, l, at[side], :] = line

    def next_y(j, which, lo, hi):
        for l in which:
            y_ref[j, l, lo:hi] = m_ref[l, lo:hi] * v_ref[j, l, lo:hi]

    def next_ends(j, lo, hi):
        for k in range(2):
            l = ends[k]
            v = v_ref[j + 1, l, lo:hi] - face_ref[SLOT[f"t{j}"], k, lo:hi]
            v_ref[j + 1, l, lo:hi] = v
            y_ref[j + 1, l, lo:hi] = m_ref[l, lo:hi] * v

    load_k.wait()
    for l in order:
        d = 6.0 + d_ref[l]
        d_ref[l] = d
        m_ref[l] = 1.0 / (d * d + 6.0)
    load_r.wait()
    for l in order:
        y_ref[0, l] = m_ref[l] * v_ref[0, l]
    y, t = y_ref.at[0], t_ref.at[0]
    for side in range(2):
        stage("y0", y, side)
        stage("d", d_ref, side)
        for k in range(2):
            corner_out[side, k, 0] = y[ends[k], at[side], :]
    for l in order:
        t[l] = local_k(y, l)
    for side in range(2):
        stage("t0", t, side)
    pl.semaphore_wait(barrier, greetings)
    for side in range(2):
        corners(side, 0, 1)
    faces("y0", y, 0, 0, cut)
    for side in range(2):
        edges("y0", y, side)
    faces("t0", t, 0, 0, cut)
    for side in range(2):
        edges("t0", t, side)
    faces("y0", y, 1, cut, rows)
    faces("t0", t, 1, cut, rows)
    for side in range(2):
        edges("d", d_ref, side)
    mu.append(dot(lambda l: v_ref[0, l], lambda l: y_ref[0, l]))
    dots[0, 0] = dot(lambda l: v_ref[0, l], lambda l: v_ref[0, l])
    y, t = y_ref.at[1], t_ref.at[1]
    spans = [
        [(0, cut), (0, cut_y), (0, cut_t), (0, cut_w)],
        [(cut, rows), (cut_y, rows), (cut_t, rows), (cut_w, rows)],
    ]
    for part in range(2):
        side, (span, span_y, span_t, span_w) = part, spans[part]
        wait(edge_in.at[pl.ds(SLOT["y0"], 2), side], edge_sem("y0", side))
        if part == 0:
            faces("d", d_ref, 0, 0, rows)
        wait_faces("y0", part, *span)
        full_t(0, *span)
        next_v(0, *span_y)
        wait(corner_in.at[side, :, 0], corner_recv.at[side])
        next_rows(0, 0, (side,))
        next_y(1, inside, *span_y)
        wait_faces("t0", part, *span)
        next_ends(0, *span_y)
        faces("y1", y, part, *span_y)
        edges("y1", y, side)
        for k in range(2):
            corner_out[side, k, OUTER] = y[ends[k], at[side], :]
            corner_out[side, k, INNER_ROW] = y[ends[k], at_second[side], :]
            corner_out[side, k, INNER_LAYER] = y[seconds[k], at[side], :]
        corners(side, OUTER, 3, False)
        lo, hi = span_t
        for l in order:
            t[l, lo:hi] = local_k(y, l, lo, hi)
        faces("t1", t, part, lo, hi)
        edges("t1", t, side)
        for k in range(2):
            corner_out[side, k, PARTIAL] = t[ends[k], at[side], :]
        corners(side, PARTIAL, 1, False)
        lo, hi = span_w
        for l in order:
            w_ref[l, lo:hi] = local_k(t, l, lo, hi)
        faces("w1", w_ref, part, lo, hi)
        edges("w1", w_ref, side)
    mu.append(dot(lambda l: f_ref[l], lambda l: f_ref[l]))
    mu.append(dot(lambda l: v_ref[1, l], lambda l: y_ref[1, l]))
    for i in range(2):
        dots[i, 1] = dot(lambda l: v_ref[i, l], lambda l: v_ref[1, l])
    wait_edges("y1")
    wait_faces("y1")
    full_t(1, 0, rows)
    next_v(1, 0, rows)
    mu.append(dot(lambda l: f_ref[l], lambda l: f_ref[l]))
    wait(edge_in.at[pl.ds(SLOT["d"], 2)], edge_sem("t1", 0))
    wait(corner_in.at[:, :, pl.ds(OUTER, 4)], corner_recv.at[2])
    next_rows(1, OUTER, range(2))
    next_y(2, inside, 0, rows)
    past = {
        (k, side): corner(k, side, PARTIAL) - (edge("y1", side, ends[k]) + face_ref[SLOT["y1"], k, at[side], :])
        for k in range(2)
        for side in range(2)
    }
    edge_part = {}
    for side in range(2):
        lines = []
        for l in range(layers):
            line = y_ref[1, l, at[side], :]
            for k in range(2):
                if l == ends[k]:
                    line = line + corner(k, side, OUTER)
            lines.append(line)
        for l in range(layers):
            beside = across(lines[l])
            if l > 0:
                beside = beside + lines[l - 1]
            if l < layers - 1:
                beside = beside + lines[l + 1]
            part = beside - edge("d", side, l) * lines[l] - f_ref[l, at[side], :]
            for k in range(2):
                if l == ends[k]:
                    part = part + (corner(k, side, INNER_ROW) - past[k, side])
            edge_part[side, l] = part
    wait_faces("d")
    for k in range(2):
        pre_ref[k] = y_ref[1, ends[k]]
        for side in range(2):
            pre_ref[k, at[side], :] = pre_ref[k, at[side], :] + corner(k, side, OUTER)
        a = pre_ref[k]
        d = face("d", k)
        near_m[k] = 1.0 / (d * d + 6.0)
        pre_ref[k] = lateral(a) - d * a - f_ref[ends[k]]
        for side in range(2):
            pre_ref[k, at[side], :] = pre_ref[k, at[side], :] + (corner(k, side, INNER_LAYER) - past[k, side])
    wait_faces("t1")
    next_ends(1, 0, rows)
    y, t = y_ref.at[2], t_ref.at[2]
    for side in range(2):
        for k in range(2):
            corner_out[side, k, LAST] = y[ends[k], at[side], :]
        corners(side, LAST, 1)
    for l in order:
        t[l] = local_k(y, l)
        f_ref[l] = t[l]
    for side in range(2):
        edges("t2", t, side)
    faces("t2", t, 0, 0, rows)
    mu.append(dot(lambda l: v_ref[2, l], lambda l: y_ref[2, l]))
    for i in range(3):
        dots[i, 2] = dot(lambda l: v_ref[i, l], lambda l: v_ref[2, l])
    wait_edges("w1")
    for side in range(2):
        for l in range(layers):
            d = edge("d", side, l)
            y = (edge("w1", side, l) + edge_part[side, l]) / (d * d + 6.0)
            f_ref[l, at[side], :] = f_ref[l, at[side], :] - y
    part = sum(f_ref[l] * f_ref[l] for l in inside)
    line = sums_line(mu, dots, slots.shape[-1])
    wait_faces("w1")
    for k in range(2):
        t = f_ref[ends[k]] - near_m[k] * (face("w1", k) + pre_ref[k])
        part = part + t * t
    mu.append(tile_sum(part))
    lane = lax.broadcasted_iota(jnp.int32, line.shape, 1)
    slots[me] = jnp.where(lane == place(("mu", 2 * ITERS - 1)), mu[-1], line)
    start_sums(slots, sum_send, sum_recv, me, nx, ny)
    for k in range(2):
        f_ref[ends[k]] = f_ref[ends[k]] - near_m[k] * (face("w1", k) + pre_ref[k])
    next_v(2, 0, rows)
    for side in range(2):
        wait_edges("t2", side)
        wait(corner_in.at[side, :, LAST], corner_recv.at[side])
    next_rows(2, LAST, range(2))
    wait_faces("t2")
    for k in range(2):
        v_ref[3, ends[k]] = v_ref[3, ends[k]] - face("t2", k)

    wait(face_ref, face_send)
    wait(edge_in, edge_send)
    wait(corner_in, corner_send)
    all_slots = slots.at[pl.ds(0, count - 1)]
    pltpu.make_async_copy(all_slots, all_slots, sum_send).wait()
    pltpu.make_async_copy(all_slots, all_slots, sum_recv).wait()
    total = jnp.sum(slots[...], axis=0)

    def whole(name):
        n = place(name)
        return jnp.broadcast_to(total[:, n : n + 1], total.shape)

    mu = [whole(("mu", i)) for i in range(2 * ITERS)]
    got = {name: whole(name) for name in dots}
    sol, res, norms = coefficients(mu, got, float(cells))
    for k, value in enumerate(norms + sol[:ITERS] + res[1:]):
        coef_ref[k] = value


def place(name):
    names = [("mu", i) for i in range(2 * ITERS)]
    names += [(i, j) for j in range(ITERS) for i in range(j + 1)]
    return names.index(name)


def sums_line(mu, dots, size):
    lane = lax.broadcasted_iota(jnp.int32, (1, size), 1)
    line = jnp.zeros(lane.shape, jnp.float32)
    named = [(("mu", i), value) for i, value in enumerate(mu)] + list(dots.items())
    for name, value in named:
        line = jnp.where(lane == place(name), value, line)
    return line


def start_sums(slots, sum_send, sum_recv, me, nx, ny):
    def send(x, y):
        pltpu.make_async_remote_copy(
            src_ref=slots.at[me],
            dst_ref=slots.at[me],
            send_sem=sum_send,
            recv_sem=sum_recv,
            device_id=(x, y),
            device_id_type=MESH,
        ).start()

    ix, iy = lax.axis_index("gx"), lax.axis_index("gy")
    for k in range(ny - 1):
        send(ix, jnp.where(iy <= k, k + 1, k))

    def send_line(k, carry):
        x = jnp.where(ix <= k, k + 1, k)
        for y in range(ny):
            send(x, y)
        return carry

    lax.fori_loop(0, nx - 1, send_line, 0, unroll=nx * ny <= 64)


def finish(coef, v_ref, y_ref, sol_ref, res_ref, norms_ref):
    cols = v_ref.shape[-1]
    lines = [jnp.concatenate([coef[k]] * (cols // coef.shape[-1]), axis=1) for k in range(3 * ITERS)]
    half = v_ref.shape[1] // pl.num_programs(0)
    for n in range(half):
        l = pl.program_id(0) * half + n
        sol = lines[ITERS] * y_ref[0, l]
        res = v_ref[0, l]
        for i in range(1, ITERS):
            sol = sol + lines[ITERS + i] * y_ref[i, l]
        for i in range(1, ITERS + 1):
            res = res + lines[2 * ITERS + i - 1] * v_ref[i, l]
        sol_ref[n] = sol
        res_ref[n] = res
    lane = lax.broadcasted_iota(jnp.int32, coef.shape[1:], 1)
    line = coef[0]
    for i in range(1, ITERS):
        line = jnp.where(lane == i, coef[i], line)
    norms_ref[...] = line[0, :ITERS]


def body(right_side, kappa_sq):
    nx, ny = lax.axis_size("gx"), lax.axis_size("gy")
    shape = right_side.shape
    layers, rows, cols = shape
    cells = nx * layers * ny * rows * cols
    f32 = jnp.float32
    dma = pltpu.SemaphoreType.DMA
    whole = pl.BlockSpec(memory_space=pltpu.VMEM)
    out = pl.pallas_call(
        functools.partial(kernel, nx, ny, cells),
        out_shape=(
            pltpu.VMEM((ITERS + 1,) + shape, f32),
            pltpu.VMEM((ITERS,) + shape, f32),
            pltpu.VMEM((3 * ITERS, 1, 128), f32),
        ),
        in_specs=[pl.BlockSpec(memory_space=pl.ANY)] * 2,
        out_specs=(whole, whole, whole),
        scratch_shapes=[
            pltpu.VMEM((ITERS,) + shape, f32),
            pltpu.VMEM(shape, f32),
            pltpu.VMEM(shape, f32),
            pltpu.VMEM(shape, f32),
            pltpu.VMEM(shape, f32),
            pltpu.VMEM((2, rows, cols), f32),
            pltpu.VMEM((2, rows, cols), f32),
            pltpu.VMEM((len(FACES), 2, rows, cols), f32),
            pltpu.VMEM((len(FACES), 2, layers, 1, cols), f32),
            pltpu.VMEM((len(FACES), 2, layers, 1, cols), f32),
            pltpu.VMEM((2, 2, 6, 1, cols), f32),
            pltpu.VMEM((2, 2, 6, 1, cols), f32),
            pltpu.VMEM((nx * ny, 1, 128), f32),
            dma((2,)),
            dma((len(ARRIVALS),)),
            dma(()),
            dma((len(ARRIVALS) - 3,)),
            dma((3,)),
            dma(()),
            dma(()),
        ],
        compiler_params=pltpu.CompilerParams(collective_id=0, has_side_effects=True),
    )(right_side, kappa_sq)
    return pl.pallas_call(
        finish,
        out_shape=(
            jax.ShapeDtypeStruct(shape, f32),
            jax.ShapeDtypeStruct(shape, f32),
            jax.ShapeDtypeStruct((ITERS,), f32),
        ),
        grid=(2,),
        in_specs=[whole, whole, whole],
        out_specs=(pl.BlockSpec((layers // 2, rows, cols), lambda h: (h, 0, 0)),) * 2 + (whole,),
    )(*(pltpu.with_memory_space_constraint(x, pltpu.VMEM) for x in (out[2], out[0], out[1])))


def solution(mesh):
    return jax.shard_map(
        body,
        mesh=mesh,
        in_specs=(P("gx", "gy", None), P("gx", "gy", None)),
        out_specs=(P("gx", "gy", None), P("gx", "gy", None), P()),
        check_vma=False,
    )
```
